256 devices in a mesh: team: 16 (over z, core), member: 16 (over x, y).
Axes of the slice: x: 4, y: 4, z: 8, core: 2. Of those that a mesh axis runs over, the one named last changes fastest.
Arguments:
- state_start: float32 [24, 1024, 2048], P(None, 'team', 'member'), may hold values from -6 to 6
- state_section: float32 [24, 1024, 2048], P(None, 'team', 'member'), may hold values from -6 to 6
- velocity: float32 [2, 1024, 2048], P(None, 'team', 'member'), may hold values from -3 to 3
- diffusivity: float32 [24], replicated, may hold values from 0.05 to 0.5
- flame_cells: int32 [256, 128], P(('team', 'member')), may hold values from 0 to 8191, as said below
- block_team: int32 [256, 1], replicated, may hold values from 0 to 15; in each aligned block of 16 rows (0 to 15, 16 to 31, ...) at most 2 rows name the same one
- w_in: bfloat16 [16, 16, 1600, 24], P('team', 'member'), may hold values from -1.25 to 1.25
- w_mid: bfloat16 [16, 16, 800, 1600], P('team', 'member'), may hold values from -0.15625 to 0.15625
- w_low: bfloat16 [16, 16, 400, 800], P('team', 'member'), may hold values from -0.21875 to 0.21875
- w_out: bfloat16 [16, 16, 24, 400], P('team', 'member'), may hold values from -0.3125 to 0.3125
Outputs:
- source_rates: float32 [24, 1024, 2048], P(None, 'team', 'member')
- new_state: float32 [24, 1024, 2048], P(None, 'team', 'member')
The draws below stay inside these ranges and needn't reach their ends.
Inputs may be any that keep to these rules, and one draw needn't show every extreme that they name: `flame_cells`: the 128 entries of the rows of one device (rows d * 1 to d + 1 - 1) are distinct cells of that device's tile, given as i * 128 + j. `block_team`: in each aligned block of 16 rows (the flame blocks of one index of team) no regime appears more than 2 times.
All inputs are finite; a program needn't handle non-finite values.
Results may differ from the reference program's by a relative error of at most 0.0017.
The reference program's roundings to bfloat16 on the way (of `inputs`, `hidden_one`, `hidden_two` and `hidden_three`) count: a program that leaves them out, or rounds other values in their place, can miss the bound.
Values may be sent and summed in bfloat16 or wider, within the bound.
No kernel may reach another device: no remote copies, remote signals or barrier semaphores. Data moves between devices by JAX's collectives and lax.ppermute only.
A program may use at most 64 MiB of HBM per device.

```python
import math
import jax
import jax.numpy as jnp
import numpy as np
from jax import lax

F = 24
H1 = 1600
H2 = 800
H3 = 400
BLOCK = 128
BLK_DEV = 1
CAP = 2
CX = 64
CY = 128
NX = 1024
NY = 2048
REGIMES = 16
NETS = 16
BLOCKS = 256
N_TEAM = 16
N_MEMBER = 16


def draw_flame_cells(key, part):
    owners = N_TEAM * N_MEMBER
    key_list = jax.random.split(jax.random.fold_in(key, 11), owners)

    def pick_cells(subkey):
        shuffled = jax.random.permutation(subkey, CX * CY)
        return shuffled[:BLK_DEV * BLOCK]
    flame_rows = jax.vmap(pick_cells)(key_list)
    return flame_rows.reshape(BLK_DEV * owners, BLOCK).astype(jnp.int32)


def level_of(rng, extent, cuts, low, top_value):
    def one(axis_at, blocks):
        steps = jax.random.uniform(jax.random.fold_in(jax.random.fold_in(rng, 6), axis_at), (blocks,), jnp.float32, low / len(cuts), top_value / len(cuts))
        return jnp.repeat(jnp.exp(steps), extent[axis_at] // blocks).reshape((-1,) + (1,) * (len(extent) - axis_at - 1))

    level = one(*cuts[0])
    for cut in cuts[1:]:
        level = level * one(*cut)
    return level


def shared_out(key, own, number, rows, number_of, top, most, lean):
    ranking = jax.random.permutation(key, number_of)
    packed, ordinary = portions_of(number_of, rows * top, most, lean, True), portions_of(number_of, rows * top, most, lean, False)
    places = jnp.arange(number_of)

    def named(tallies, rotation):
        used = int((tallies > 0).sum())
        fixed = max(1, used // 4)
        moved = fixed + (places - fixed + rotation * (used - fixed)) % max(1, number_of - fixed)
        return jnp.zeros((number_of,), jnp.int32).at[ranking[jnp.where(places < fixed, places, moved)]].set(jnp.asarray(tallies, jnp.int32))

    tallies = jnp.where(number % 4 == 0, named(packed, number // 4), named(ordinary, number - number // 4 - 1))
    mixed = jax.random.permutation(jax.random.fold_in(own, 3), number_of)
    source_of, sink = mixed[0:number_of // 2 * 2:2], mixed[1:number_of // 2 * 2:2]
    margin = jnp.minimum(tallies[source_of] - 1, most - tallies[sink]) // 2
    margin = jnp.where((source_of == ranking[0]) | (sink == ranking[0]) | (tallies[sink] == 0), 0, jnp.maximum(margin, 0))
    moved = jax.random.randint(jax.random.fold_in(own, 4), (number_of // 2,), 0, 1 << 20) % (margin + 1)
    tallies = tallies.at[source_of].add(-moved).at[sink].add(moved)
    items = jnp.searchsorted(jnp.cumsum(tallies), jnp.arange(rows * top), side="right").astype(jnp.int32)
    listing = items.reshape(top, rows).T
    listing = listing[jax.random.permutation(jax.random.fold_in(own, 1), rows)]
    rotation = jax.random.randint(jax.random.fold_in(own, 2), (rows, 1), 0, top)
    return jnp.take_along_axis(listing, (jnp.arange(top)[None, :] + rotation) % top, axis=1)


def portions_of(amount, total, bound, lean, full):
    portions = [(1 << 20) // math.isqrt(standing ** lean) + 1 for standing in range(1, amount + 1)]
    largest = bound if full else min(bound, max(-(-total // amount), total * portions[0] // sum(portions)))
    least = 1 if total - largest >= amount - 1 else 0
    counts, spare = [largest] + [least] * (amount - 1), total - largest - least * (amount - 1)
    while spare > 0:
        candidates = [i for i in range(1, amount) if counts[i] < largest] or [i for i in range(1, amount) if counts[i] < bound]
        pool, remaining = sum([portions[i] for i in candidates]), spare
        for i in candidates:
            extra = min(bound - counts[i], max(1, remaining * portions[i] // pool), spare)
            counts[i] = counts[i] + extra
            spare = spare - extra
    return np.array(counts)


def normal_values(own_key, shape, width, bound, cuts=(), held_as=jnp.bfloat16):
    array = width * jax.random.normal(own_key, shape, jnp.float32)
    if cuts:
        array = array * level_of(own_key, shape, cuts, -0.22, 0.18)
    return jnp.clip(array, -bound, bound).astype(held_as)


def setup_inputs(seed: int = 0) -> dict:
    streams_of = jax.random.split(jax.random.key(seed), 11)
    state_start = normal_values(streams_of[0], (F, NX, NY), 1.0, 6.0, ((1, 16), (2, 16)), jnp.float32)
    state_section = normal_values(streams_of[1], (F, NX, NY), 1.0, 6.0, ((1, 16), (2, 16)), jnp.float32)
    velocity = normal_values(streams_of[2], (2, NX, NY), 0.7, 3.0, ((1, 16), (2, 16)), jnp.float32)
    diffusivity = jnp.clip(jnp.exp(jax.random.uniform(streams_of[3], (F,), jnp.float32, math.log(0.05), math.log(0.5))), 0.05, 0.5)
    flame_cells = draw_flame_cells(jax.random.fold_in(streams_of[10], 71), 0)
    block_team_keys = jax.random.split(jax.random.fold_in(streams_of[5], 1), BLOCKS // (N_MEMBER * BLK_DEV))
    block_team_turns = jax.random.permutation(jax.random.fold_in(streams_of[5], 3), BLOCKS // (N_MEMBER * BLK_DEV))
    block_team = jax.vmap(lambda own, number: shared_out(jax.random.fold_in(streams_of[5], 2), own, number, N_MEMBER * BLK_DEV, N_TEAM, 1, CAP, 2))(block_team_keys, block_team_turns).reshape((BLOCKS, 1))
    w_in = normal_values(streams_of[6], (REGIMES, NETS, H1, F), F ** -0.5, 1.25, ((0, 16), (1, 16)))
    w_mid = normal_values(streams_of[7], (REGIMES, NETS, H2, H1), H1 ** -0.5, 0.15625, ((0, 16), (1, 16)))
    w_low = normal_values(streams_of[8], (REGIMES, NETS, H3, H2), H2 ** -0.5, 0.21875, ((0, 16), (1, 16)))
    w_out = normal_values(streams_of[9], (REGIMES, NETS, F, H3), H3 ** -0.5, 0.3125, ((0, 16), (1, 16)))
    return dict(state_start=state_start, state_section=state_section, velocity=velocity, diffusivity=diffusivity, flame_cells=flame_cells, block_team=block_team, w_in=w_in, w_mid=w_mid, w_low=w_low, w_out=w_out)


TIME_STEP = 0.25


def flow_operator(state_section, velocity, diffusivity):
    plus_x = jnp.roll(state_section, -1, axis=1)
    minus_x = jnp.roll(state_section, 1, axis=1)
    plus_y = jnp.roll(state_section, -1, axis=2)
    minus_y = jnp.roll(state_section, 1, axis=2)
    spread = diffusivity[:, None, None] * (plus_x + minus_x + plus_y + minus_y - 4.0 * state_section)
    advect = 0.5 * velocity[0][None] * (plus_x - minus_x) + 0.5 * velocity[1][None] * (plus_y - minus_y)
    return spread - advect


def network_sum(states, weight_in, weight_mid, weight_low, weight_out):
    highest = lax.Precision.HIGHEST
    layer_one = jnp.einsum("nhf,fk->nhk", weight_in.astype(jnp.float32), states.astype(jnp.float32), precision=highest)
    hidden_one = jax.nn.silu(layer_one).astype(jnp.bfloat16)
    layer_two = jnp.einsum("nih,nhk->nik", weight_mid.astype(jnp.float32), hidden_one.astype(jnp.float32), precision=highest)
    hidden_two = jax.nn.silu(layer_two).astype(jnp.bfloat16)
    layer_three = jnp.einsum("nji,nik->njk", weight_low.astype(jnp.float32), hidden_two.astype(jnp.float32), precision=highest)
    hidden_three = jax.nn.silu(layer_three).astype(jnp.bfloat16)
    return jnp.einsum("nfj,njk->fk", weight_out.astype(jnp.float32), hidden_three.astype(jnp.float32), precision=highest)


def reference(state_start, state_section, velocity, diffusivity, flame_cells, block_team, w_in, w_mid, w_low, w_out):
    block_ids = jnp.arange(BLOCKS, dtype=jnp.int32)
    owners = block_ids // BLK_DEV
    grid_x = ((owners // N_MEMBER)[:, None] * CX + flame_cells // CY).astype(jnp.int32)
    grid_y = ((owners % N_MEMBER)[:, None] * CY + flame_cells % CY).astype(jnp.int32)
    gathered = jnp.transpose(state_section[:, grid_x, grid_y], (1, 0, 2)).astype(jnp.bfloat16)

    def block_rates(inputs):
        states, regime = inputs
        return network_sum(states, w_in[regime], w_mid[regime], w_low[regime], w_out[regime])

    block_values = lax.map(block_rates, (gathered, block_team[:, 0]))
    source_rates = jnp.zeros(state_section.shape, jnp.float32).at[:, grid_x, grid_y].add(jnp.transpose(block_values, (1, 0, 2)))
    flow = flow_operator(state_section, velocity, diffusivity)
    new_state = 0.75 * state_start + 0.25 * (state_section + TIME_STEP * (flow + source_rates))
    return source_rates, new_state
```

```python
import jax
import jax.numpy as jnp
from jax import lax
from jax.experimental import pallas as pl
from jax.experimental.pallas import tpu as pltpu
from jax.sharding import Mesh, PartitionSpec as P

BF = jnp.bfloat16
F32 = jnp.float32
I32 = jnp.int32
TIME_STEP = 0.25
VM = pl.BlockSpec(memory_space=pltpu.VMEM)
SM = pl.BlockSpec(memory_space=pltpu.SMEM)
HB = pl.BlockSpec(memory_space=pl.ANY)
PARAMS = pltpu.CompilerParams(vmem_limit_bytes=56 * 2**20)

SRC, POS, OWN, SIB, N_OWN, N_SIB, CORE = 0, 32, 64, 80, 96, 97, 98


def dot(a, b, dims=((1,), (0,))):
    return lax.dot_general(a, b, (dims, ((), ())), preferred_element_type=F32)


def silu(x):
    h = 0.5 * x
    return (h * jnp.tanh(h) + h).astype(BF)


def iota(shape, dim):
    return lax.broadcasted_iota(I32, shape, dim)


def table_kernel(ids, team_ref, out):
    z, c, q = ids[0], ids[1], ids[2]
    n = team_ref.shape[1]
    across = jnp.broadcast_to(team_ref[...].astype(F32), (n, n))
    down = across.T
    row, lane = iota((n, n), 0), iota((n, n), 1)
    before = (across == down) & (lane < row)
    rank = jnp.sum(jnp.where(before, 1.0, 0.0), axis=1, keepdims=True).astype(I32)
    near = before & ((lane // 32) == (row // 32))
    local = jnp.sum(jnp.where(near, 1.0, 0.0), axis=1, keepdims=True).astype(I32)
    shape = (n, 128)
    g = down[:, :128].astype(I32)
    rank = jnp.broadcast_to(rank, shape)
    local = jnp.broadcast_to(local, shape)
    b, s = iota(shape, 0), iota(shape, 1)
    core = (rank + g) & 1
    slot = (g & 1) * 2 + (local >> 1)
    place = (g >> 1) * 4 + slot
    here = (b >> 5) == z
    mine = core == c
    own = mine & (g == 2 * z + c)
    sib = mine & (g == 2 * z + 1 - c)
    arrives = (b >> 5) * 4 + slot
    zero = jnp.zeros(shape, I32)
    value = jnp.where((s < POS) & here & mine & (place == s), b & 31, zero)
    value = jnp.where((s >= POS) & (s < OWN) & here & ((b & 31) == s - POS), place, value)
    value = jnp.where((s >= OWN) & (s < SIB) & own & ((rank >> 1) == s - OWN), arrives, value)
    value = jnp.where((s >= SIB) & (s < N_OWN) & sib & ((rank >> 1) == s - SIB), arrives, value)
    value = jnp.where((s == N_OWN) & own, 1, value)
    value = jnp.where((s == N_SIB) & sib, 1, value)
    value = jnp.where((s == CORE) & (b == (2 * z + c) * 16 + q), core, value)
    out[...] = jnp.sum(value.astype(F32), axis=0, keepdims=True).astype(I32)


def front_kernel(cells, state, blocks, x_low, x_high, y_edges):
    fields, rows, cols = state.shape
    width = cells.shape[1]
    column = cells[...] & (cols - 1)
    line = cells[...] >> (cols.bit_length() - 1)
    picks = jnp.where(iota((cols, width), 0) == column, 1.0, 0.0).astype(BF)
    flat = state[...].astype(BF).reshape(fields * rows, cols)
    found = dot(flat, picks).reshape(fields, rows, width)
    at_row = (iota((rows, width), 0) == line)[None]
    own = jnp.sum(jnp.where(at_row, found, 0.0), axis=1).astype(BF)
    for k in range(blocks.shape[0]):
        blocks[k] = own
    x_low[...] = state[:, 0, :].astype(BF)
    x_high[...] = state[:, rows - 1, :].astype(BF)
    e, j = iota((16, cols), 0), iota((16, cols), 1)
    ends = jnp.where(((e == 0) & (j == 0)) | ((e == 1) & (j == cols - 1)), 1.0, 0.0).astype(BF)
    y_edges[...] = dot(ends, flat, ((1,), (1,)))[0:2].astype(BF)


def select_kernel(base, table, rows, out):
    for k in range(out.shape[0]):
        out[k] = rows[table[0, base + k]]


def network_kernel(table, x, *refs):
    hbm, out = refs[:8], refs[8]
    scratch, sems = refs[9:13], refs[13]
    copies = [
        [pltpu.make_async_copy(hbm[4 * w + k], scratch[k].at[w], sems.at[w, k]) for k in range(4)]
        for w in range(2)
    ]
    for w in range(2):
        for copy in copies[w]:
            copy.start()
    for w, (first, count) in enumerate(((OWN, N_OWN), (SIB, N_SIB))):
        for copy in copies[w]:
            copy.wait()
        n = table[0, count]

        def step(k, _, w=w, first=first, n=n):
            at = [table[0, first + jnp.minimum(4 * k + i, n - 1)] for i in range(4)]
            states = jnp.concatenate([x[i] for i in at], axis=1)
            one = silu(dot(scratch[0][w], states, ((0,), (0,))))
            two = silu(dot(scratch[1][w], one))
            three = silu(dot(scratch[2][w], two))
            rates = dot(scratch[3][w], three)
            for i, a in enumerate(at):
                out[a] = rates[:, i * 128 : (i + 1) * 128]
            return 0

        lax.fori_loop(0, (n + 3) // 4, step, 0)


def base_kernel(diff, start, state, velocity, up, down, y_edges, out):
    fields, rows, cols = state.shape
    e, j = iota((2, cols), 0), iota((2, cols), 1)
    ends = jnp.where(((e == 0) & (j == 0)) | ((e == 1) & (j == cols - 1)), 1.0, 0.0).astype(BF)
    sides = dot(y_edges[...], ends, ((0,), (0,))).reshape(fields, rows, cols)
    row, lane = iota((rows, cols), 0), iota((rows, cols), 1)
    half_x, half_y = 0.5 * velocity[0], 0.5 * velocity[1]
    for f in range(fields):
        u = state[f]
        plus_x = jnp.where(row == rows - 1, down[f : f + 1].astype(F32), pltpu.roll(u, rows - 1, 0))
        minus_x = jnp.where(row == 0, up[f : f + 1].astype(F32), pltpu.roll(u, 1, 0))
        plus_y = jnp.where(lane == cols - 1, sides[f], pltpu.roll(u, cols - 1, 1))
        minus_y = jnp.where(lane == 0, sides[f], pltpu.roll(u, 1, 1))
        flow = diff[f] * (plus_x + minus_x + plus_y + minus_y - 4.0 * u)
        flow = flow - half_x * (plus_x - minus_x) - half_y * (plus_y - minus_y)
        out[f] = 0.75 * start[f] + 0.25 * (u + TIME_STEP * flow)


def final_kernel(table, cells, parts, base, source, new):
    fields, rows, cols = base.shape
    width = cells.shape[1]
    first = table[0, CORE] * 16
    rates = parts[first]
    for n in range(1, 16):
        rates = rates + parts[first + n]
    high = rates.astype(BF).astype(F32)
    low = rates - high
    column = cells[...] & (cols - 1)
    line = cells[...] >> (cols.bit_length() - 1)
    at_row = iota((rows, width), 0) == line
    at_col = jnp.where(iota((cols, width), 0) == column, 1.0, 0.0).astype(BF)
    at_col = jnp.concatenate([at_col, at_col], axis=1)
    for f in range(fields):
        left = jnp.where(at_row, high[f : f + 1], 0.0)
        right = jnp.where(at_row, low[f : f + 1], 0.0)
        spread = jnp.concatenate([left, right], axis=1).astype(BF)
        placed = dot(spread, at_col, ((1,), (1,)))
        source[f] = placed
        new[f] = base[f] + (0.25 * TIME_STEP) * placed


def call(body, out_shape, in_specs, out_specs=None, scratch=(), name=None):
    if out_specs is None:
        out_specs = jax.tree.map(lambda _: VM, out_shape)
    return pl.pallas_call(
        body, out_shape=out_shape, in_specs=in_specs, out_specs=out_specs,
        scratch_shapes=scratch, compiler_params=PARAMS, name=name,
    )


def shards(start, state, velocity, diffusivity, cells, block_team, w_in, w_mid, w_low, w_out):
    fields, rows, cols = state.shape
    width = cells.shape[1]
    sds = jax.ShapeDtypeStruct
    members = lax.axis_size("member")
    teams = lax.axis_size("z") * lax.axis_size("core")
    up = [(i, (i + 1) % 16) for i in range(16)]
    back = [(b, a) for a, b in up]
    swap = [(0, 1), (1, 0)]
    plane = ("core", "member")
    line = ("z", "core")

    ids = jnp.stack([lax.axis_index(a) for a in ("z", "core", "member")]).astype(I32)
    weights = [w_in[0, 0].T, w_mid[0, 0], w_low[0, 0], w_out[0, 0]]
    partner = [lax.ppermute(w, "core", swap) for w in weights]

    blocks, x_low, x_high, y_edges = call(
        front_kernel,
        (sds((2 * members, fields, width), BF), sds((fields, cols), BF), sds((fields, cols), BF),
         sds((2, fields * rows), BF)),
        [VM, VM], name="front",
    )(cells, state)
    gathered = lax.all_to_all(blocks, plane, 0, 0, tiled=True)
    table = call(table_kernel, sds((1, 128), I32), [SM, VM], name="table")(ids, block_team.T)
    outgoing = call(
        lambda *r: select_kernel(SRC, *r), sds((32, fields, width), BF), [SM, VM], name="select"
    )(table, gathered)
    incoming = lax.all_to_all(outgoing, "z", 0, 0, tiled=True)

    from_up = lax.ppermute(x_high, line, up)
    from_down = lax.ppermute(x_low, line, back)
    from_left = lax.ppermute(y_edges[1:2], "member", up)
    from_right = lax.ppermute(y_edges[0:1], "member", back)

    produced = call(
        network_kernel, sds((32, fields, width), F32), [SM, VM] + [HB] * 8,
        scratch=[pltpu.VMEM((2, *w.shape), BF) for w in weights] + [pltpu.SemaphoreType.DMA((2, 4))],
        name="networks",
    )(table, incoming, *weights, *partner)
    returned = lax.all_to_all(produced, "z", 0, 0, tiled=True)
    base = call(
        base_kernel, sds(state.shape, F32), [SM] + [VM] * 6, name="base"
    )(diffusivity, start, state, velocity, from_up, from_down,
      jnp.concatenate([from_left, from_right], axis=0))
    terms = call(
        lambda *r: select_kernel(POS, *r), sds((32, fields, width), F32), [SM, VM], name="pick"
    )(table, returned)
    parts = lax.all_to_all(terms, plane, 0, 0, tiled=True)
    return call(
        final_kernel, (sds(state.shape, F32), sds(state.shape, F32)), [SM, VM, VM, VM], name="final"
    )(table, cells, parts, base)


def solution(mesh):
    team, member = mesh.devices.shape
    own_mesh = Mesh(mesh.devices.reshape(team // 2, 2, member), ("z", "core", "member"))
    line = ("z", "core")
    tile = P(None, line, "member")
    weight = P(line, "member", None, None)
    return jax.shard_map(
        shards,
        mesh=own_mesh,
        in_specs=(tile, tile, tile, P(), P((*line, "member"), None), P(), weight, weight, weight, weight),
        out_specs=(tile, tile),
        check_vma=False,
    )
```

```python
import jax
import jax.numpy as jnp
from jax import lax
from jax.experimental import pallas as pl
from jax.experimental.pallas import tpu as pltpu
from jax.sharding import Mesh, PartitionSpec as P

BF = jnp.bfloat16
F32 = jnp.float32
I32 = jnp.int32
TIME_STEP = 0.25
VM = pl.BlockSpec(memory_space=pltpu.VMEM)
SM = pl.BlockSpec(memory_space=pltpu.SMEM)

ANY = pl.BlockSpec(memory_space=pl.ANY)

SRC, POS, OWN, SIB, N_OWN, N_SIB = 0, 32, 48, 64, 80, 81


def dot(a, b, dims=((1,), (0,))):
    return lax.dot_general(a, b, (dims, ((), ())), preferred_element_type=F32)


def silu(x):
    return (x * lax.logistic(x)).astype(BF)


def in_hbm(array):
    return pltpu.with_memory_space_constraint(array, pltpu.HBM)


def iota(shape, dim):
    return lax.broadcasted_iota(I32, shape, dim)


def table_kernel(team_ref, out):
    z, c = lax.axis_index("z"), lax.axis_index("core")
    n = team_ref.shape[1]
    across = jnp.broadcast_to(team_ref[...].astype(F32), (n, n))
    down = across.T
    row, lane = iota((n, n), 0), iota((n, n), 1)
    before = (across == down) & (lane < row)
    rank = jnp.sum(jnp.where(before, 1.0, 0.0), axis=1, keepdims=True).astype(I32)
    shape = (n, 128)
    g = down[:, :128].astype(I32)
    rank = jnp.broadcast_to(rank, shape)
    b, s = iota(shape, 0), iota(shape, 1)
    core = (rank + g) & 1
    place = ((g >> 1) * 2 + core) * 2 + (g & 1)
    arrives = (b >> 4) * 2 + (g & 1)
    here = (b >> 4) == 2 * z + c
    own = (core == c) & (g == 2 * z + c)
    sib = (core == c) & (g == 2 * z + 1 - c)
    value = jnp.where((s < POS) & here & (place == s), b & 15, jnp.zeros(shape, I32))
    value = jnp.where((s >= POS) & (s < OWN) & here & ((b & 15) == s - POS), place, value)
    value = jnp.where((s >= OWN) & (s < SIB) & own & ((rank >> 1) == s - OWN), arrives, value)
    value = jnp.where((s >= SIB) & (s < N_OWN) & sib & ((rank >> 1) == s - SIB), arrives, value)
    value = jnp.where((s == N_OWN) & own, 1, value)
    value = jnp.where((s == N_SIB) & sib, 1, value)
    out[...] = jnp.sum(value.astype(F32), axis=0, keepdims=True).astype(I32)


def front_kernel(cells, state, blocks, x_low, x_high, y_edges):
    fields, rows, cols = state.shape
    width = cells.shape[1]
    column = cells[...] & (cols - 1)
    line = cells[...] >> (cols.bit_length() - 1)
    picks = jnp.where(iota((cols, width), 0) == column, 1.0, 0.0).astype(BF)
    flat = state[...].astype(BF).reshape(fields * rows, cols)
    found = dot(flat, picks).reshape(fields, rows, width)
    at_row = (iota((rows, width), 0) == line)[None]
    own = jnp.sum(jnp.where(at_row, found, 0.0), axis=1).astype(BF)
    for k in range(blocks.shape[0]):
        blocks[k] = own
    x_low[...] = state[:, 0, :].astype(BF)
    x_high[...] = state[:, rows - 1, :].astype(BF)
    e, j = iota((16, cols), 0), iota((16, cols), 1)
    ends = jnp.where(((e == 0) & (j == 0)) | ((e == 1) & (j == cols - 1)), 1.0, 0.0).astype(BF)
    y_edges[...] = dot(ends, flat, ((1,), (1,)))[0:2].astype(BF)


def select_kernel(base, table, rows, out):
    for k in range(out.shape[0]):
        out[k] = rows[table[0, base + k]]


def network_kernel(table, x, *refs):
    out, rates, sems, load_sems = refs[8], refs[9], refs[10], refs[11]
    own, partner = refs[12:16], [refs[4], refs[16], refs[6], refs[7]]
    loads = [pltpu.make_async_copy(refs[k], own[k], load_sems.at[k]) for k in range(4)]
    loads.append(pltpu.make_async_copy(refs[5], refs[16], load_sems.at[4]))
    for load in loads:
        load.start()

    def copy_of(g, i, a):
        return pltpu.make_async_copy(rates.at[g, i], out.at[a], sems.at[g, i])

    done = 0
    for weights, first, count in ((own, OWN, N_OWN), (partner, SIB, N_SIB)):
        w_in, w_mid, w_low, w_out = weights
        n = table[0, count]
        for load in loads[:4] if weights is own else loads[4:]:
            load.wait()

        def step(k, _, w_in=w_in, w_mid=w_mid, w_low=w_low, w_out=w_out, first=first, n=n, done=done):
            at = [table[0, first + jnp.minimum(4 * k + i, n - 1)] for i in range(4)]
            states = jnp.concatenate([x[i] for i in at], axis=1)
            one = silu(dot(w_in[...], states, ((0,), (0,))))
            two = silu(dot(w_mid[...], one))
            three = silu(dot(w_low[...], two))
            found = dot(w_out[...], three)
            for i, a in enumerate(at):
                rates[done + k, i] = found[:, i * 128 : (i + 1) * 128]

                @pl.when(4 * k + i < n)
                def _(i=i, a=a):
                    copy_of(done + k, i, a).start()

            return 0

        lax.fori_loop(0, (n + 3) // 4, step, 0)
        done = done + (n + 3) // 4

    done = 0
    for count in (N_OWN, N_SIB):
        n = table[0, count]

        def finish(k, _, n=n, done=done):
            for i in range(4):

                @pl.when(4 * k + i < n)
                def _(i=i):
                    copy_of(done + k, i, 0).wait()

            return 0

        lax.fori_loop(0, (n + 3) // 4, finish, 0)
        done = done + (n + 3) // 4


def base_kernel(diff, start, state, velocity, up, down, y_edges, out):
    fields, rows, cols = state.shape
    e, j = iota((2, cols), 0), iota((2, cols), 1)
    ends = jnp.where(((e == 0) & (j == 0)) | ((e == 1) & (j == cols - 1)), 1.0, 0.0).astype(BF)
    sides = dot(y_edges[...], ends, ((0,), (0,))).reshape(fields, rows, cols)
    row, lane = iota((rows, cols), 0), iota((rows, cols), 1)
    half_x, half_y = 0.5 * velocity[0], 0.5 * velocity[1]
    for f in range(fields):
        u = state[f]
        plus_x = jnp.where(row == rows - 1, down[f : f + 1].astype(F32), pltpu.roll(u, rows - 1, 0))
        minus_x = jnp.where(row == 0, up[f : f + 1].astype(F32), pltpu.roll(u, 1, 0))
        plus_y = jnp.where(lane == cols - 1, sides[f], pltpu.roll(u, cols - 1, 1))
        minus_y = jnp.where(lane == 0, sides[f], pltpu.roll(u, 1, 1))
        flow = diff[f] * (plus_x + minus_x + plus_y + minus_y - 4.0 * u)
        flow = flow - half_x * (plus_x - minus_x) - half_y * (plus_y - minus_y)
        out[f] = 0.75 * start[f] + 0.25 * (u + TIME_STEP * flow)


def final_kernel(cells, parts, base, source, new, source_tile, new_tile, sems):
    fields, rows, cols = base.shape
    width = cells.shape[1]
    rates = parts[0]
    for n in range(1, parts.shape[0]):
        rates = rates + parts[n]
    high = rates.astype(BF).astype(F32)
    low = rates - high
    column = cells[...] & (cols - 1)
    line = cells[...] >> (cols.bit_length() - 1)
    at_row = iota((rows, width), 0) == line
    at_col = jnp.where(iota((cols, width), 0) == column, 1.0, 0.0).astype(BF)
    at_col = jnp.concatenate([at_col, at_col], axis=1)
    some = fields // sems.shape[1]
    copies = []
    for k in range(sems.shape[1]):
        spread = []
        for f in range(k * some, (k + 1) * some):
            left = jnp.where(at_row, high[f : f + 1], 0.0)
            right = jnp.where(at_row, low[f : f + 1], 0.0)
            spread.append(jnp.concatenate([left, right], axis=1).astype(BF))
        placed = dot(jnp.concatenate(spread, axis=0), at_col, ((1,), (1,)))
        placed = placed.reshape(some, rows, cols)
        part = pl.ds(k * some, some)
        source_tile[part] = placed
        new_tile[part] = base[part] + (0.25 * TIME_STEP) * placed
        for i, (tile, out) in enumerate(((source_tile, source), (new_tile, new))):
            copies.append(pltpu.make_async_copy(tile.at[part], out.at[part], sems.at[i, k]))
            copies[-1].start()
    for copy in copies:
        copy.wait()


def call(body, out_shape, in_specs, out_specs=None, scratch=(), name=None, mib=8):
    if out_specs is None:
        out_specs = jax.tree.map(lambda _: VM, out_shape)
    return pl.pallas_call(
        body, out_shape=out_shape, in_specs=in_specs, out_specs=out_specs,
        scratch_shapes=scratch, compiler_params=pltpu.CompilerParams(vmem_limit_bytes=mib * 2**20), name=name,
    )


def shards(start, state, velocity, diffusivity, cells, block_team, w_in, w_mid, w_low, w_out):
    fields, rows, cols = state.shape
    width = cells.shape[1]
    sds = jax.ShapeDtypeStruct
    members = lax.axis_size("member")
    teams = lax.axis_size("z") * lax.axis_size("core")
    up = [(i, (i + 1) % 16) for i in range(16)]
    back = [(b, a) for a, b in up]
    swap = [(0, 1), (1, 0)]
    line = ("z", "core")

    weights = [w_in[0, 0].T, w_mid[0, 0], w_low[0, 0], w_out[0, 0]]
    partner = [lax.ppermute(w, "core", swap) for w in weights]

    blocks, x_low, x_high, y_edges = call(
        front_kernel,
        (sds((members, fields, width), BF), sds((fields, cols), BF), sds((fields, cols), BF),
         sds((2, fields * rows), BF)),
        [VM, VM], name="front",
    )(cells, state)
    gathered = lax.all_to_all(blocks, "member", 0, 0, tiled=True)
    table = call(table_kernel, sds((1, 128), I32), [VM], name="table")(block_team.T)
    outgoing = call(
        lambda *r: select_kernel(SRC, *r), sds((2 * teams, fields, width), BF), [SM, VM], name="select"
    )(table, gathered)
    incoming = lax.all_to_all(outgoing, line, 0, 0, tiled=True)

    from_up = lax.ppermute(x_high, line, up)
    from_down = lax.ppermute(x_low, line, back)
    from_left = lax.ppermute(y_edges[1:2], "member", up)
    from_right = lax.ppermute(y_edges[0:1], "member", back)
    incoming, from_up, from_down, from_left, from_right = lax.optimization_barrier(
        (incoming, from_up, from_down, from_left, from_right)
    )

    produced = call(
        network_kernel, sds((2 * teams, fields, width), F32), [SM, VM] + [ANY] * 4 + [VM, ANY, VM, VM], ANY,
        scratch=[pltpu.VMEM((8, 4, fields, width), F32), pltpu.SemaphoreType.DMA((8, 4)), pltpu.SemaphoreType.DMA((5,))]
        + [pltpu.VMEM(w.shape, BF) for w in (*weights, weights[1])],
        name="networks", mib=24,
    )(table, incoming, *[in_hbm(w) for w in weights], partner[0], in_hbm(partner[1]), *partner[2:])
    returned = lax.all_to_all(produced, line, 0, 0, tiled=True)
    base = call(
        base_kernel, sds(state.shape, F32), [SM] + [VM] * 6, name="base"
    )(diffusivity, start, state, velocity, from_up, from_down,
      jnp.concatenate([from_left, from_right], axis=0))
    returned, base = lax.optimization_barrier((returned, base))
    terms = call(
        lambda *r: select_kernel(POS, *r), sds((members, fields, width), F32), [SM, VM], name="pick"
    )(table, returned)
    parts = lax.all_to_all(terms, "member", 0, 0, tiled=True)
    return call(
        final_kernel, (sds(state.shape, F32), sds(state.shape, F32)), [VM, VM, VM], (ANY, ANY),
        scratch=[pltpu.VMEM(state.shape, F32), pltpu.VMEM(state.shape, F32), pltpu.SemaphoreType.DMA((2, 3))],
        name="final",
    )(cells, parts, base)


def solution(mesh):
    team, member = mesh.devices.shape
    own_mesh = Mesh(mesh.devices.reshape(team // 2, 2, member), ("z", "core", "member"))
    line = ("z", "core")
    tile = P(None, line, "member")
    weight = P(line, "member", None, None)
    return jax.shard_map(
        shards,
        mesh=own_mesh,
        in_specs=(tile, tile, tile, P(), P((*line, "member"), None), P(), weight, weight, weight, weight),
        out_specs=(tile, tile),
        check_vma=False,
    )
```

```python
import jax
import jax.numpy as jnp
from jax import lax
from jax.experimental import pallas as pl
from jax.experimental.pallas import tpu as pltpu
from jax.sharding import Mesh, PartitionSpec as P

BF = jnp.bfloat16
F32 = jnp.float32
I32 = jnp.int32
TIME_STEP = 0.25
VM = pl.BlockSpec(memory_space=pltpu.VMEM)
SM = pl.BlockSpec(memory_space=pltpu.SMEM)

ANY = pl.BlockSpec(memory_space=pl.ANY)

SRC, POS, OWN, SIB, N_OWN, N_SIB = 0, 32, 48, 64, 80, 81


def dot(a, b, dims=((1,), (0,))):
    return lax.dot_general(a, b, (dims, ((), ())), preferred_element_type=F32)


def silu(x):
    return (x * lax.logistic(x)).astype(BF)


def in_hbm(array):
    return pltpu.with_memory_space_constraint(array, pltpu.HBM)


def iota(shape, dim):
    return lax.broadcasted_iota(I32, shape, dim)


def table_kernel(team_ref, out):
    z, c = lax.axis_index("z"), lax.axis_index("core")
    n = team_ref.shape[1]
    across = jnp.broadcast_to(team_ref[...].astype(F32), (n, n))
    down = across.T
    row, lane = iota((n, n), 0), iota((n, n), 1)
    before = (across == down) & (lane < row)
    rank = jnp.sum(jnp.where(before, 1.0, 0.0), axis=1, keepdims=True).astype(I32)
    shape = (n, 128)
    g = down[:, :128].astype(I32)
    rank = jnp.broadcast_to(rank, shape)
    b, s = iota(shape, 0), iota(shape, 1)
    core = (rank + g) & 1
    place = ((g >> 1) * 2 + core) * 2 + (g & 1)
    arrives = (b >> 4) * 2 + (g & 1)
    here = (b >> 4) == 2 * z + c
    own = (core == c) & (g == 2 * z + c)
    sib = (core == c) & (g == 2 * z + 1 - c)
    value = jnp.where((s < POS) & here & (place == s), b & 15, jnp.zeros(shape, I32))
    value = jnp.where((s >= POS) & (s < OWN) & here & ((b & 15) == s - POS), place, value)
    value = jnp.where((s >= OWN) & (s < SIB) & own & ((rank >> 1) == s - OWN), arrives, value)
    value = jnp.where((s >= SIB) & (s < N_OWN) & sib & ((rank >> 1) == s - SIB), arrives, value)
    value = jnp.where((s == N_OWN) & own, 1, value)
    value = jnp.where((s == N_SIB) & sib, 1, value)
    out[...] = jnp.sum(value.astype(F32), axis=0, keepdims=True).astype(I32)


def front_kernel(cells_hbm, state_hbm, blocks, x_low, x_high, y_low, y_high, cells, state, own, sems, out_sems):
    fields, rows, cols = state.shape
    width = cells.shape[1]
    parts = sems.shape[0] - 1
    some = fields // parts
    loads = [pltpu.make_async_copy(cells_hbm, cells, sems.at[parts])]
    for k in range(parts):
        at = pl.ds(k * some, some)
        loads.append(pltpu.make_async_copy(state_hbm.at[at], state.at[at], sems.at[k]))
    for load in loads:
        load.start()
    loads[0].wait()
    column = cells[...] & (cols - 1)
    line = cells[...] >> (cols.bit_length() - 1)
    picks = jnp.where(iota((cols, width), 0) == column, 1.0, 0.0).astype(BF)
    at_row = (iota((rows, width), 0) == line)[None]
    e, j = iota((16, cols), 0), iota((16, cols), 1)
    ends = jnp.where(((e == 0) & (j == 0)) | ((e == 1) & (j == cols - 1)), 1.0, 0.0).astype(BF)
    found_in = []
    for k in range(parts):
        loads[k + 1].wait()
        values = state[k * some : (k + 1) * some].astype(BF)
        flat = values.reshape(some * rows, cols)
        found = dot(flat, picks).reshape(some, rows, width)
        found_in.append(jnp.sum(jnp.where(at_row, found, 0.0), axis=1))
        sides = dot(ends, flat, ((1,), (1,))).astype(BF)
        at = slice(k * some * rows, (k + 1) * some * rows)
        y_low[:, at], y_high[:, at] = sides[0:1], sides[1:2]
    own[...] = jnp.concatenate(found_in, axis=0).astype(BF)
    sends = [pltpu.make_async_copy(own, blocks.at[k], out_sems.at[k]) for k in range(blocks.shape[0])]
    for send in sends:
        send.start()
    x_low[...] = state[:, 0, :].astype(BF)
    x_high[...] = state[:, rows - 1, :].astype(BF)
    for send in sends:
        send.wait()


def select_kernel(base, table, rows, out):
    for k in range(out.shape[0]):
        out[k] = rows[table[0, base + k]]


def network_kernel(table, x, *refs):
    out, rates, sems, load_sems = refs[8], refs[9], refs[10], refs[11]
    partner, own = [refs[4], refs[5], refs[16], refs[7]], refs[12:16]
    first_load = pltpu.make_async_copy(refs[6], refs[16], load_sems.at[4])
    loads = [pltpu.make_async_copy(refs[k], own[k], load_sems.at[k]) for k in range(4)]
    for load in (first_load, *loads):
        load.start()
    first_load.wait()

    def copy_of(g, i, a):
        return pltpu.make_async_copy(rates.at[g, i], out.at[a], sems.at[g, i])

    done = 0
    for weights, first, count in ((partner, SIB, N_SIB), (own, OWN, N_OWN)):
        w_in, w_mid, w_low, w_out = weights
        n = table[0, count]
        if weights is own:
            for load in loads:
                load.wait()

        def step(k, _, w_in=w_in, w_mid=w_mid, w_low=w_low, w_out=w_out, first=first, n=n, done=done):
            at = [table[0, first + jnp.minimum(4 * k + i, n - 1)] for i in range(4)]
            states = jnp.concatenate([x[i] for i in at], axis=1)
            one = silu(dot(w_in[...], states, ((0,), (0,))))
            two = silu(dot(w_mid[...], one))
            three = silu(dot(w_low[...], two))
            found = dot(w_out[...], three)
            for i, a in enumerate(at):
                rates[done + k, i] = found[:, i * 128 : (i + 1) * 128]

                @pl.when(4 * k + i < n)
                def _(i=i, a=a):
                    copy_of(done + k, i, a).start()

            return 0

        lax.fori_loop(0, (n + 3) // 4, step, 0)
        done = done + (n + 3) // 4

    done = 0
    for count in (N_SIB, N_OWN):
        n = table[0, count]

        def finish(k, _, n=n, done=done):
            for i in range(4):

                @pl.when(4 * k + i < n)
                def _(i=i):
                    copy_of(done + k, i, 0).wait()

            return 0

        lax.fori_loop(0, (n + 3) // 4, finish, 0)
        done = done + (n + 3) // 4


def base_kernel(diff, start, state, velocity, up, down, left, right, out):
    fields, rows, cols = state.shape
    e, j = iota((2, cols), 0), iota((2, cols), 1)
    ends = jnp.where(((e == 0) & (j == 0)) | ((e == 1) & (j == cols - 1)), 1.0, 0.0).astype(BF)
    edges = jnp.concatenate([left[...], right[...]], axis=0)
    sides = dot(edges, ends, ((0,), (0,))).reshape(fields, rows, cols)
    row, lane = iota((rows, cols), 0), iota((rows, cols), 1)
    half_x, half_y = 0.5 * velocity[0], 0.5 * velocity[1]
    for f in range(fields):
        u = state[f]
        plus_x = jnp.where(row == rows - 1, down[f : f + 1].astype(F32), pltpu.roll(u, rows - 1, 0))
        minus_x = jnp.where(row == 0, up[f : f + 1].astype(F32), pltpu.roll(u, 1, 0))
        plus_y = jnp.where(lane == cols - 1, sides[f], pltpu.roll(u, cols - 1, 1))
        minus_y = jnp.where(lane == 0, sides[f], pltpu.roll(u, 1, 1))
        flow = diff[f] * (plus_x + minus_x + plus_y + minus_y - 4.0 * u)
        flow = flow - half_x * (plus_x - minus_x) - half_y * (plus_y - minus_y)
        out[f] = 0.75 * start[f] + 0.25 * (u + TIME_STEP * flow)


def final_kernel(cells, parts, base, source, new, source_tile, new_tile, sems):
    fields, rows, cols = base.shape
    width = cells.shape[1]
    rates = parts[0]
    for n in range(1, parts.shape[0]):
        rates = rates + parts[n]
    high = rates.astype(BF).astype(F32)
    low = rates - high
    column = cells[...] & (cols - 1)
    line = cells[...] >> (cols.bit_length() - 1)
    at_row = iota((rows, width), 0) == line
    at_col = jnp.where(iota((cols, width), 0) == column, 1.0, 0.0).astype(BF)
    at_col = jnp.concatenate([at_col, at_col], axis=1)
    some = fields // sems.shape[1]
    copies = []
    for k in range(sems.shape[1]):
        spread = []
        for f in range(k * some, (k + 1) * some):
            left = jnp.where(at_row, high[f : f + 1], 0.0)
            right = jnp.where(at_row, low[f : f + 1], 0.0)
            spread.append(jnp.concatenate([left, right], axis=1).astype(BF))
        placed = dot(jnp.concatenate(spread, axis=0), at_col, ((1,), (1,)))
        placed = placed.reshape(some, rows, cols)
        part = pl.ds(k * some, some)
        source_tile[part] = placed
        new_tile[part] = base[part] + (0.25 * TIME_STEP) * placed
        for i, (tile, out) in enumerate(((source_tile, source), (new_tile, new))):
            copies.append(pltpu.make_async_copy(tile.at[part], out.at[part], sems.at[i, k]))
            copies[-1].start()
    for copy in copies:
        copy.wait()


def call(body, out_shape, in_specs, out_specs=None, scratch=(), name=None, mib=8):
    if out_specs is None:
        out_specs = jax.tree.map(lambda _: VM, out_shape)
    return pl.pallas_call(
        body, out_shape=out_shape, in_specs=in_specs, out_specs=out_specs,
        scratch_shapes=scratch, compiler_params=pltpu.CompilerParams(vmem_limit_bytes=mib * 2**20), name=name,
    )


def shards(start, state, velocity, diffusivity, cells, block_team, w_in, w_mid, w_low, w_out):
    fields, rows, cols = state.shape
    width = cells.shape[1]
    sds = jax.ShapeDtypeStruct
    members = lax.axis_size("member")
    teams = lax.axis_size("z") * lax.axis_size("core")
    up = [(i, (i + 1) % 16) for i in range(16)]
    back = [(b, a) for a, b in up]
    swap = [(0, 1), (1, 0)]
    line = ("z", "core")

    weights = [w_in[0, 0].T, w_mid[0, 0], w_low[0, 0], w_out[0, 0]]
    partner = [lax.ppermute(w, "core", swap) for w in weights]

    edge = sds((1, fields * rows), BF)
    blocks, x_low, x_high, y_low, y_high = call(
        front_kernel,
        (sds((members, fields, width), BF), sds((fields, cols), BF), sds((fields, cols), BF), edge, edge),
        [ANY, ANY], (ANY, VM, VM, VM, VM),
        scratch=[pltpu.VMEM(cells.shape, I32), pltpu.VMEM(state.shape, F32), pltpu.VMEM((fields, width), BF),
                 pltpu.SemaphoreType.DMA((4,)), pltpu.SemaphoreType.DMA((members,))],
        name="front",
    )(in_hbm(cells), in_hbm(state))
    gathered = lax.all_to_all(blocks, "member", 0, 0, tiled=True)
    gathered, partner[0], partner[3] = lax.optimization_barrier((gathered, partner[0], partner[3]))
    table = call(table_kernel, sds((1, 128), I32), [VM], name="table")(block_team.T)
    outgoing = call(
        lambda *r: select_kernel(SRC, *r), sds((2 * teams, fields, width), BF), [SM, VM], name="select"
    )(table, gathered)
    incoming = lax.all_to_all(outgoing, line, 0, 0, tiled=True)

    produced = call(
        network_kernel, sds((2 * teams, fields, width), F32), [SM, VM] + [ANY] * 4 + [VM, VM, ANY, VM], ANY,
        scratch=[pltpu.VMEM((8, 4, fields, width), F32), pltpu.SemaphoreType.DMA((8, 4)), pltpu.SemaphoreType.DMA((5,))]
        + [pltpu.VMEM(w.shape, BF) for w in (*weights, weights[2])],
        name="networks", mib=24,
    )(table, incoming, *[in_hbm(w) for w in weights], partner[0], partner[1], in_hbm(partner[2]), partner[3])
    produced, x_low, x_high, y_low, y_high = lax.optimization_barrier((produced, x_low, x_high, y_low, y_high))
    returned = lax.all_to_all(produced, line, 0, 0, tiled=True)
    halos = (
        lax.ppermute(x_high, line, up),
        lax.ppermute(x_low, line, back),
        lax.ppermute(y_high, "member", up),
        lax.ppermute(y_low, "member", back),
    )
    base = call(base_kernel, sds(state.shape, F32), [SM] + [VM] * 7, name="base")(
        diffusivity, in_hbm(start), in_hbm(state), in_hbm(velocity), *halos
    )
    returned, base = lax.optimization_barrier((returned, base))
    terms = call(
        lambda *r: select_kernel(POS, *r), sds((members, fields, width), F32), [SM, VM], name="pick"
    )(table, returned)
    parts = lax.all_to_all(terms, "member", 0, 0, tiled=True)
    return call(
        final_kernel, (sds(state.shape, F32), sds(state.shape, F32)), [VM, VM, VM], (ANY, ANY),
        scratch=[pltpu.VMEM(state.shape, F32), pltpu.VMEM(state.shape, F32), pltpu.SemaphoreType.DMA((2, 3))],
        name="final",
    )(cells, parts, base)


def solution(mesh):
    team, member = mesh.devices.shape
    own_mesh = Mesh(mesh.devices.reshape(team // 2, 2, member), ("z", "core", "member"))
    line = ("z", "core")
    tile = P(None, line, "member")
    weight = P(line, "member", None, None)
    return jax.shard_map(
        shards,
        mesh=own_mesh,
        in_specs=(tile, tile, tile, P(), P((*line, "member"), None), P(), weight, weight, weight, weight),
        out_specs=(tile, tile),
        check_vma=False,
    )
```

```python
import jax
import jax.numpy as jnp
from jax import lax
from jax.experimental import pallas as pl
from jax.experimental.pallas import tpu as pltpu
from jax.sharding import Mesh, PartitionSpec as P

BF = jnp.bfloat16
F32 = jnp.float32
I32 = jnp.int32
TIME_STEP = 0.25
VM = pl.BlockSpec(memory_space=pltpu.VMEM)
SM = pl.BlockSpec(memory_space=pltpu.SMEM)

ANY = pl.BlockSpec(memory_space=pl.ANY)

SRC, POS, OWN, SIB, N_OWN, N_SIB = 0, 32, 48, 64, 80, 81


def dot(a, b, dims=((1,), (0,))):
    return lax.dot_general(a, b, (dims, ((), ())), preferred_element_type=F32)


def silu(x):
    return (x * lax.logistic(x)).astype(BF)


def in_hbm(array):
    return pltpu.with_memory_space_constraint(array, pltpu.HBM)


def iota(shape, dim):
    return lax.broadcasted_iota(I32, shape, dim)


def table_kernel(team_ref, out):
    z, c = lax.axis_index("z"), lax.axis_index("core")
    n = team_ref.shape[1]
    across = jnp.broadcast_to(team_ref[...].astype(F32), (n, n))
    down = across.T
    row, lane = iota((n, n), 0), iota((n, n), 1)
    before = (across == down) & (lane < row)
    rank = jnp.sum(jnp.where(before, 1.0, 0.0), axis=1, keepdims=True).astype(I32)
    shape = (n, 128)
    g = down[:, :128].astype(I32)
    rank = jnp.broadcast_to(rank, shape)
    b, s = iota(shape, 0), iota(shape, 1)
    core = (rank + g) & 1
    place = ((g >> 1) * 2 + core) * 2 + (g & 1)
    arrives = (b >> 4) * 2 + (g & 1)
    here = (b >> 4) == 2 * z + c
    own = (core == c) & (g == 2 * z + c)
    sib = (core == c) & (g == 2 * z + 1 - c)
    value = jnp.where((s < POS) & here & (place == s), b & 15, jnp.zeros(shape, I32))
    value = jnp.where((s >= POS) & (s < OWN) & here & ((b & 15) == s - POS), place, value)
    value = jnp.where((s >= OWN) & (s < SIB) & own & ((rank >> 1) == s - OWN), arrives, value)
    value = jnp.where((s >= SIB) & (s < N_OWN) & sib & ((rank >> 1) == s - SIB), arrives, value)
    value = jnp.where((s == N_OWN) & own, 1, value)
    value = jnp.where((s == N_SIB) & sib, 1, value)
    out[...] = jnp.sum(value.astype(F32), axis=0, keepdims=True).astype(I32)


def front_kernel(cells_hbm, state_hbm, blocks, x_low, x_high, y_low, y_high, cells, state, own, sems, out_sems):
    fields, rows, cols = state.shape
    width = cells.shape[1]
    parts = sems.shape[0] - 1
    some = fields // parts
    loads = [pltpu.make_async_copy(cells_hbm, cells, sems.at[parts])]
    for k in range(parts):
        at = pl.ds(k * some, some)
        loads.append(pltpu.make_async_copy(state_hbm.at[at], state.at[at], sems.at[k]))
    for load in loads:
        load.start()
    loads[0].wait()
    column = cells[...] & (cols - 1)
    line = cells[...] >> (cols.bit_length() - 1)
    picks = jnp.where(iota((cols, width), 0) == column, 1.0, 0.0).astype(BF)
    at_row = (iota((rows, width), 0) == line)[None]
    e, j = iota((16, cols), 0), iota((16, cols), 1)
    ends = jnp.where(((e == 0) & (j == 0)) | ((e == 1) & (j == cols - 1)), 1.0, 0.0).astype(BF)
    found_in = []
    for k in range(parts):
        loads[k + 1].wait()
        values = state[k * some : (k + 1) * some].astype(BF)
        flat = values.reshape(some * rows, cols)
        found = dot(flat, picks).reshape(some, rows, width)
        found_in.append(jnp.sum(jnp.where(at_row, found, 0.0), axis=1))
    own[...] = jnp.concatenate(found_in, axis=0).astype(BF)
    sends = [pltpu.make_async_copy(own, blocks.at[k], out_sems.at[k]) for k in range(blocks.shape[0])]
    for send in sends:
        send.start()
    x_low[...] = state[:, 0, :].astype(BF)
    x_high[...] = state[:, rows - 1, :].astype(BF)
    sides = dot(ends, state[...].astype(BF).reshape(fields * rows, cols), ((1,), (1,))).astype(BF)
    y_low[...], y_high[...] = sides[0:1], sides[1:2]
    for send in sends:
        send.wait()


def select_kernel(base, table, rows, out):
    for k in range(out.shape[0]):
        out[k] = rows[table[0, base + k]]


def network_kernel(table, x, *refs):
    out, rates, sems, load_sems = refs[8], refs[9], refs[10], refs[11]
    partner, own = [refs[4], refs[5], refs[16], refs[7]], refs[12:16]
    first_load = pltpu.make_async_copy(refs[6], refs[16], load_sems.at[4])
    loads = [pltpu.make_async_copy(refs[k], own[k], load_sems.at[k]) for k in range(4)]
    for load in (first_load, *loads):
        load.start()
    first_load.wait()

    def copy_of(w, p, a):
        return pltpu.make_async_copy(rates.at[w, p], out.at[a], sems.at[w, p])

    def group(weights, w, first, n, start, size):
        w_in, w_mid, w_low, w_out = weights
        at = [table[0, first + jnp.minimum(start + i, n - 1)] for i in range(size)]
        states = jnp.concatenate([x[i] for i in at], axis=1)
        one = silu(dot(w_in[...], states, ((0,), (0,))))
        two = silu(dot(w_mid[...], one))
        three = silu(dot(w_low[...], two))
        found = dot(w_out[...], three)
        for i, a in enumerate(at):
            rates[w, start + i] = found[:, i * 128 : (i + 1) * 128]

            @pl.when(start + i < n)
            def _(i=i, a=a):
                copy_of(w, start + i, a).start()

    counts = table[0, N_SIB], table[0, N_OWN]
    for w, (weights, first) in enumerate(((partner, SIB), (own, OWN))):
        n = counts[w]
        if w == 1:
            for load in loads:
                load.wait()
        full = (n + 3) // 8

        def step(k, _, weights=weights, w=w, first=first, n=n):
            group(weights, w, first, n, 8 * k, 8)
            return 0

        lax.fori_loop(0, full, step, 0)

        @pl.when(n > 8 * full)
        def _(weights=weights, w=w, first=first, n=n, full=full):
            group(weights, w, first, n, 8 * full, 4)

    for w in range(2):
        for p in range(16):

            @pl.when(p < counts[w])
            def _(w=w, p=p):
                copy_of(w, p, 0).wait()


def base_kernel(diff, start, state, velocity, up, down, left, right, out):
    fields, rows, cols = state.shape
    e, j = iota((2, cols), 0), iota((2, cols), 1)
    ends = jnp.where(((e == 0) & (j == 0)) | ((e == 1) & (j == cols - 1)), 1.0, 0.0).astype(BF)
    edges = jnp.concatenate([left[...], right[...]], axis=0)
    sides = dot(edges, ends, ((0,), (0,))).reshape(fields, rows, cols)
    row, lane = iota((rows, cols), 0), iota((rows, cols), 1)
    half_x, half_y = 0.5 * velocity[0], 0.5 * velocity[1]
    for f in range(fields):
        u = state[f]
        plus_x = jnp.where(row == rows - 1, down[f : f + 1].astype(F32), pltpu.roll(u, rows - 1, 0))
        minus_x = jnp.where(row == 0, up[f : f + 1].astype(F32), pltpu.roll(u, 1, 0))
        plus_y = jnp.where(lane == cols - 1, sides[f], pltpu.roll(u, cols - 1, 1))
        minus_y = jnp.where(lane == 0, sides[f], pltpu.roll(u, 1, 1))
        flow = diff[f] * (plus_x + minus_x + plus_y + minus_y - 4.0 * u)
        flow = flow - half_x * (plus_x - minus_x) - half_y * (plus_y - minus_y)
        out[f] = 0.75 * start[f] + 0.25 * (u + TIME_STEP * flow)


def final_kernel(cells, parts, base, source, new, source_tile, new_tile, sems):
    fields, rows, cols = base.shape
    width = cells.shape[1]
    rates = parts[0]
    for n in range(1, parts.shape[0]):
        rates = rates + parts[n]
    high = rates.astype(BF).astype(F32)
    low = rates - high
    column = cells[...] & (cols - 1)
    line = cells[...] >> (cols.bit_length() - 1)
    at_row = iota((rows, width), 0) == line
    at_col = jnp.where(iota((cols, width), 0) == column, 1.0, 0.0).astype(BF)
    at_col = jnp.concatenate([at_col, at_col], axis=1)
    some = fields // sems.shape[1]
    copies = []
    for k in range(sems.shape[1]):
        spread = []
        for f in range(k * some, (k + 1) * some):
            left = jnp.where(at_row, high[f : f + 1], 0.0)
            right = jnp.where(at_row, low[f : f + 1], 0.0)
            spread.append(jnp.concatenate([left, right], axis=1).astype(BF))
        placed = dot(jnp.concatenate(spread, axis=0), at_col, ((1,), (1,)))
        placed = placed.reshape(some, rows, cols)
        part = pl.ds(k * some, some)
        source_tile[part] = placed
        new_tile[part] = base[part] + (0.25 * TIME_STEP) * placed
        for i, (tile, out) in enumerate(((source_tile, source), (new_tile, new))):
            copies.append(pltpu.make_async_copy(tile.at[part], out.at[part], sems.at[i, k]))
            copies[-1].start()
    for copy in copies:
        copy.wait()


def call(body, out_shape, in_specs, out_specs=None, scratch=(), name=None, mib=8):
    if out_specs is None:
        out_specs = jax.tree.map(lambda _: VM, out_shape)
    return pl.pallas_call(
        body, out_shape=out_shape, in_specs=in_specs, out_specs=out_specs,
        scratch_shapes=scratch, compiler_params=pltpu.CompilerParams(vmem_limit_bytes=mib * 2**20), name=name,
    )


def shards(start, state, velocity, diffusivity, cells, block_team, w_in, w_mid, w_low, w_out):
    fields, rows, cols = state.shape
    width = cells.shape[1]
    sds = jax.ShapeDtypeStruct
    members = lax.axis_size("member")
    teams = lax.axis_size("z") * lax.axis_size("core")
    up = [(i, (i + 1) % 16) for i in range(16)]
    back = [(b, a) for a, b in up]
    swap = [(0, 1), (1, 0)]
    line = ("z", "core")

    weights = [w_in[0, 0].T, w_mid[0, 0], w_low[0, 0], w_out[0, 0]]
    edge = sds((1, fields * rows), BF)
    blocks, x_low, x_high, y_low, y_high = call(
        front_kernel,
        (sds((members, fields, width), BF), sds((fields, cols), BF), sds((fields, cols), BF), edge, edge),
        [ANY, ANY], (ANY, VM, VM, VM, VM),
        scratch=[pltpu.VMEM(cells.shape, I32), pltpu.VMEM(state.shape, F32), pltpu.VMEM((fields, width), BF),
                 pltpu.SemaphoreType.DMA((4,)), pltpu.SemaphoreType.DMA((members,))],
        name="front",
    )(in_hbm(cells), in_hbm(state))
    blocks, *sent = lax.optimization_barrier((blocks, *weights))
    gathered = lax.all_to_all(blocks, "member", 0, 0, tiled=True)
    partner = [lax.ppermute(w, "core", swap) for w in sent]
    from_left = lax.ppermute(y_high, "member", up)
    from_right = lax.ppermute(y_low, "member", back)
    gathered, partner[0], partner[3], from_left, from_right = lax.optimization_barrier(
        (gathered, partner[0], partner[3], from_left, from_right)
    )
    table = call(table_kernel, sds((1, 128), I32), [VM], name="table")(block_team.T)
    outgoing = call(
        lambda *r: select_kernel(SRC, *r), sds((2 * teams, fields, width), BF), [SM, VM], name="select"
    )(table, gathered)
    incoming = lax.all_to_all(outgoing, line, 0, 0, tiled=True)

    produced = call(
        network_kernel, sds((2 * teams, fields, width), F32), [SM, VM] + [ANY] * 4 + [VM, VM, ANY, VM], ANY,
        scratch=[pltpu.VMEM((2, 16, fields, width), F32), pltpu.SemaphoreType.DMA((2, 16)), pltpu.SemaphoreType.DMA((5,))]
        + [pltpu.VMEM(w.shape, BF) for w in (*weights, weights[2])],
        name="networks", mib=32,
    )(table, incoming, *[in_hbm(w) for w in weights], partner[0], partner[1], in_hbm(partner[2]), partner[3])
    produced, x_low, x_high = lax.optimization_barrier((produced, x_low, x_high))
    returned = lax.all_to_all(produced, line, 0, 0, tiled=True)
    halos = lax.ppermute(x_high, line, up), lax.ppermute(x_low, line, back), from_left, from_right
    base = call(base_kernel, sds(state.shape, F32), [SM] + [VM] * 7, name="base")(
        diffusivity, in_hbm(start), in_hbm(state), in_hbm(velocity), *halos
    )
    returned, base = lax.optimization_barrier((returned, base))
    terms = call(
        lambda *r: select_kernel(POS, *r), sds((members, fields, width), F32), [SM, VM], name="pick"
    )(table, returned)
    parts = lax.all_to_all(terms, "member", 0, 0, tiled=True)
    return call(
        final_kernel, (sds(state.shape, F32), sds(state.shape, F32)), [VM, VM, VM], (ANY, ANY),
        scratch=[pltpu.VMEM(state.shape, F32), pltpu.VMEM(state.shape, F32), pltpu.SemaphoreType.DMA((2, 3))],
        name="final",
    )(cells, parts, base)


def solution(mesh):
    team, member = mesh.devices.shape
    own_mesh = Mesh(mesh.devices.reshape(team // 2, 2, member), ("z", "core", "member"))
    line = ("z", "core")
    tile = P(None, line, "member")
    weight = P(line, "member", None, None)
    return jax.shard_map(
        shards,
        mesh=own_mesh,
        in_specs=(tile, tile, tile, P(), P((*line, "member"), None), P(), weight, weight, weight, weight),
        out_specs=(tile, tile),
        check_vma=False,
    )
```

```python
import jax
import jax.numpy as jnp
from jax import lax
from jax.experimental import pallas as pl
from jax.experimental.pallas import tpu as pltpu
from jax.sharding import Mesh, PartitionSpec as P

BF = jnp.bfloat16
F32 = jnp.float32
I32 = jnp.int32
TIME_STEP = 0.25
VM = pl.BlockSpec(memory_space=pltpu.VMEM)
SM = pl.BlockSpec(memory_space=pltpu.SMEM)

ANY = pl.BlockSpec(memory_space=pl.ANY)

SRC, POS, OWN, SIB, N_OWN, N_SIB = 0, 32, 48, 64, 80, 81


def dot(a, b, dims=((1,), (0,))):
    return lax.dot_general(a, b, (dims, ((), ())), preferred_element_type=F32)


def silu(x):
    return (x * lax.logistic(x)).astype(BF)


def in_hbm(array):
    return pltpu.with_memory_space_constraint(array, pltpu.HBM)


def iota(shape, dim):
    return lax.broadcasted_iota(I32, shape, dim)


def table_kernel(team_ref, out):
    z, c = lax.axis_index("z"), lax.axis_index("core")
    n = team_ref.shape[1]
    across = jnp.broadcast_to(team_ref[...].astype(F32), (n, n))
    down = across.T
    row, lane = iota((n, n), 0), iota((n, n), 1)
    before = (across == down) & (lane < row)
    rank = jnp.sum(jnp.where(before, 1.0, 0.0), axis=1, keepdims=True).astype(I32)
    shape = (n, 128)
    g = down[:, :128].astype(I32)
    rank = jnp.broadcast_to(rank, shape)
    b, s = iota(shape, 0), iota(shape, 1)
    core = (rank + g) & 1
    place = ((g >> 1) * 2 + core) * 2 + (g & 1)
    arrives = (b >> 4) * 2 + (g & 1)
    here = (b >> 4) == 2 * z + c
    own = (core == c) & (g == 2 * z + c)
    sib = (core == c) & (g == 2 * z + 1 - c)
    value = jnp.where((s < POS) & here & (place == s), b & 15, jnp.zeros(shape, I32))
    value = jnp.where((s >= POS) & (s < OWN) & here & ((b & 15) == s - POS), place, value)
    value = jnp.where((s >= OWN) & (s < SIB) & own & ((rank >> 1) == s - OWN), arrives, value)
    value = jnp.where((s >= SIB) & (s < N_OWN) & sib & ((rank >> 1) == s - SIB), arrives, value)
    value = jnp.where((s == N_OWN) & own, 1, value)
    value = jnp.where((s == N_SIB) & sib, 1, value)
    out[...] = jnp.sum(value.astype(F32), axis=0, keepdims=True).astype(I32)


def front_kernel(cells_hbm, state_hbm, blocks, x_low, x_high, y_low, y_high, cells, state, own, sems, out_sems):
    fields, rows, cols = state.shape
    width = cells.shape[1]
    parts = sems.shape[0] - 1
    some = fields // parts
    loads = [pltpu.make_async_copy(cells_hbm, cells, sems.at[parts])]
    for k in range(parts):
        at = pl.ds(k * some, some)
        loads.append(pltpu.make_async_copy(state_hbm.at[at], state.at[at], sems.at[k]))
    for load in loads:
        load.start()
    loads[0].wait()
    column = cells[...] & (cols - 1)
    line = cells[...] >> (cols.bit_length() - 1)
    picks = jnp.where(iota((cols, width), 0) == column, 1.0, 0.0).astype(BF)
    at_row = (iota((rows, width), 0) == line)[None]
    e, j = iota((16, cols), 0), iota((16, cols), 1)
    ends = jnp.where(((e == 0) & (j == 0)) | ((e == 1) & (j == cols - 1)), 1.0, 0.0).astype(BF)
    found_in = []
    for k in range(parts):
        loads[k + 1].wait()
        values = state[k * some : (k + 1) * some].astype(BF)
        flat = values.reshape(some * rows, cols)
        found = dot(flat, picks).reshape(some, rows, width)
        found_in.append(jnp.sum(jnp.where(at_row, found, 0.0), axis=1))
    own[...] = jnp.concatenate(found_in, axis=0).astype(BF)
    sends = [pltpu.make_async_copy(own, blocks.at[k], out_sems.at[k]) for k in range(blocks.shape[0])]
    for send in sends:
        send.start()
    x_low[...] = state[:, 0, :].astype(BF)
    x_high[...] = state[:, rows - 1, :].astype(BF)
    sides = dot(ends, state[...].astype(BF).reshape(fields * rows, cols), ((1,), (1,))).astype(BF)
    y_low[...], y_high[...] = sides[0:1], sides[1:2]
    for send in sends:
        send.wait()


def select_kernel(base, table, rows, out):
    for k in range(out.shape[0]):
        out[k] = rows[table[0, base + k]]


def network_kernel(table, x, *refs):
    out, rates, sems, load_sems = refs[8], refs[9], refs[10], refs[11]
    partner, own = [refs[4], refs[5], refs[16], refs[7]], refs[12:16]
    first_load = pltpu.make_async_copy(refs[6], refs[16], load_sems.at[4])
    loads = [pltpu.make_async_copy(refs[k], own[k], load_sems.at[k]) for k in range(4)]
    for load in (first_load, *loads):
        load.start()
    first_load.wait()

    def copy_of(w, p, a):
        return pltpu.make_async_copy(rates.at[w, p], out.at[a], sems.at[w, p])

    def group(weights, w, first, n, start, size):
        w_in, w_mid, w_low, w_out = weights
        at = [table[0, first + jnp.minimum(start + i, n - 1)] for i in range(size)]
        states = jnp.concatenate([x[i] for i in at], axis=1)
        one = silu(dot(w_in[...], states, ((0,), (0,))))
        two = silu(dot(w_mid[...], one))
        three = silu(dot(w_low[...], two))
        found = dot(w_out[...], three)
        for i, a in enumerate(at):
            rates[w, start + i] = found[:, i * 128 : (i + 1) * 128]

            @pl.when(start + i < n)
            def _(i=i, a=a):
                copy_of(w, start + i, a).start()

    counts = table[0, N_SIB], table[0, N_OWN]
    for w, (weights, first) in enumerate(((partner, SIB), (own, OWN))):
        n = counts[w]
        if w == 1:
            for load in loads:
                load.wait()
        full = (n + 3) // 8

        def step(k, _, weights=weights, w=w, first=first, n=n):
            group(weights, w, first, n, 8 * k, 8)
            return 0

        lax.fori_loop(0, full, step, 0)

        @pl.when(n > 8 * full)
        def _(weights=weights, w=w, first=first, n=n, full=full):
            group(weights, w, first, n, 8 * full, 4)

    for w in range(2):
        for p in range(16):

            @pl.when(p < counts[w])
            def _(w=w, p=p):
                copy_of(w, p, 0).wait()


def base_kernel(diff, start, state, velocity, out):
    fields, rows, cols = state.shape
    row, lane = iota((rows, cols), 0), iota((rows, cols), 1)
    half_x, half_y = 0.5 * velocity[0], 0.5 * velocity[1]
    for f in range(fields):
        u = state[f]
        plus_x = jnp.where(row == rows - 1, 0.0, pltpu.roll(u, rows - 1, 0))
        minus_x = jnp.where(row == 0, 0.0, pltpu.roll(u, 1, 0))
        plus_y = jnp.where(lane == cols - 1, 0.0, pltpu.roll(u, cols - 1, 1))
        minus_y = jnp.where(lane == 0, 0.0, pltpu.roll(u, 1, 1))
        flow = diff[f] * (plus_x + minus_x + plus_y + minus_y - 4.0 * u)
        flow = flow - half_x * (plus_x - minus_x) - half_y * (plus_y - minus_y)
        out[f] = 0.75 * start[f] + 0.25 * (u + TIME_STEP * flow)


def final_kernel(diff, cells, parts, base, velocity, up, down, left, right, source, new, source_tile, new_tile, sems):
    fields, rows, cols = base.shape
    width = cells.shape[1]
    rates = parts[0]
    for n in range(1, parts.shape[0]):
        rates = rates + parts[n]
    high = rates.astype(BF).astype(F32)
    low = rates - high
    column = cells[...] & (cols - 1)
    line = cells[...] >> (cols.bit_length() - 1)
    at_row = iota((rows, width), 0) == line
    at_col = jnp.where(iota((cols, width), 0) == column, 1.0, 0.0).astype(BF)
    at_col = jnp.concatenate([at_col, at_col], axis=1)
    some = fields // sems.shape[1]
    copies = []
    scale = 0.25 * TIME_STEP
    e, j = iota((2, cols), 0), iota((2, cols), 1)
    ends = jnp.where(((e == 0) & (j == 0)) | ((e == 1) & (j == cols - 1)), 1.0, 0.0).astype(BF)
    edges = jnp.concatenate([left[...], right[...]], axis=0)
    sides = dot(edges, ends, ((0,), (0,))).reshape(fields, rows, cols)
    lane = iota((rows, cols), 1)
    along = jnp.where(lane == 0, 0.5, -0.5) * velocity[1]
    low_x, high_x = 0.5 * velocity[0, 0:1, :], -0.5 * velocity[0, rows - 1 : rows, :]
    for k in range(sems.shape[1]):
        spread = []
        for f in range(k * some, (k + 1) * some):
            left = jnp.where(at_row, high[f : f + 1], 0.0)
            right = jnp.where(at_row, low[f : f + 1], 0.0)
            spread.append(jnp.concatenate([left, right], axis=1).astype(BF))
        placed = dot(jnp.concatenate(spread, axis=0), at_col, ((1,), (1,)))
        placed = placed.reshape(some, rows, cols)
        part = pl.ds(k * some, some)
        source_tile[part] = placed
        for f in range(some):
            g = k * some + f
            new_tile[g] = base[g] + scale * (placed[f] + (diff[g] + along) * sides[g])
            above, below = up[g : g + 1].astype(F32), down[g : g + 1].astype(F32)
            new_tile[g, 0:1] = new_tile[g, 0:1] + scale * (diff[g] + low_x) * above
            new_tile[g, rows - 1 : rows] = new_tile[g, rows - 1 : rows] + scale * (diff[g] + high_x) * below
        for i, (tile, out) in enumerate(((source_tile, source), (new_tile, new))):
            copies.append(pltpu.make_async_copy(tile.at[part], out.at[part], sems.at[i, k]))
            copies[-1].start()
    for copy in copies:
        copy.wait()


def call(body, out_shape, in_specs, out_specs=None, scratch=(), name=None, mib=8):
    if out_specs is None:
        out_specs = jax.tree.map(lambda _: VM, out_shape)
    return pl.pallas_call(
        body, out_shape=out_shape, in_specs=in_specs, out_specs=out_specs,
        scratch_shapes=scratch, compiler_params=pltpu.CompilerParams(vmem_limit_bytes=mib * 2**20), name=name,
    )


def shards(start, state, velocity, diffusivity, cells, block_team, w_in, w_mid, w_low, w_out):
    fields, rows, cols = state.shape
    width = cells.shape[1]
    sds = jax.ShapeDtypeStruct
    members = lax.axis_size("member")
    teams = lax.axis_size("z") * lax.axis_size("core")
    up = [(i, (i + 1) % 16) for i in range(16)]
    back = [(b, a) for a, b in up]
    swap = [(0, 1), (1, 0)]
    line = ("z", "core")

    weights = [w_in[0, 0].T, w_mid[0, 0], w_low[0, 0], w_out[0, 0]]
    edge = sds((1, fields * rows), BF)
    blocks, x_low, x_high, y_low, y_high = call(
        front_kernel,
        (sds((members, fields, width), BF), sds((fields, cols), BF), sds((fields, cols), BF), edge, edge),
        [ANY, ANY], (ANY, VM, VM, VM, VM),
        scratch=[pltpu.VMEM(cells.shape, I32), pltpu.VMEM(state.shape, F32), pltpu.VMEM((fields, width), BF),
                 pltpu.SemaphoreType.DMA((4,)), pltpu.SemaphoreType.DMA((members,))],
        name="front",
    )(in_hbm(cells), in_hbm(state))
    blocks, *sent = lax.optimization_barrier((blocks, *weights))
    gathered = lax.all_to_all(blocks, "member", 0, 0, tiled=True)
    partner = [lax.ppermute(w, "core", swap) for w in sent]
    gathered, partner[0], partner[3] = lax.optimization_barrier((gathered, partner[0], partner[3]))
    table = call(table_kernel, sds((1, 128), I32), [VM], name="table")(block_team.T)
    outgoing = call(
        lambda *r: select_kernel(SRC, *r), sds((2 * teams, fields, width), BF), [SM, VM], name="select"
    )(table, gathered)
    incoming = lax.all_to_all(outgoing, line, 0, 0, tiled=True)

    produced = call(
        network_kernel, sds((2 * teams, fields, width), F32), [SM, VM] + [ANY] * 4 + [VM, VM, ANY, VM], ANY,
        scratch=[pltpu.VMEM((2, 16, fields, width), F32), pltpu.SemaphoreType.DMA((2, 16)), pltpu.SemaphoreType.DMA((5,))]
        + [pltpu.VMEM(w.shape, BF) for w in (*weights, weights[2])],
        name="networks", mib=32,
    )(table, incoming, *[in_hbm(w) for w in weights], partner[0], partner[1], in_hbm(partner[2]), partner[3])
    produced, x_low, x_high, y_low, y_high = lax.optimization_barrier((produced, x_low, x_high, y_low, y_high))
    returned = lax.all_to_all(produced, line, 0, 0, tiled=True)
    halos = (
        lax.ppermute(x_high, line, up),
        lax.ppermute(x_low, line, back),
        lax.ppermute(y_high, "member", up),
        lax.ppermute(y_low, "member", back),
    )
    base = call(base_kernel, sds(state.shape, F32), [SM] + [VM] * 3, name="base")(
        diffusivity, in_hbm(start), in_hbm(state), in_hbm(velocity)
    )
    returned, base, *halos = lax.optimization_barrier((returned, base, *halos))
    terms = call(
        lambda *r: select_kernel(POS, *r), sds((members, fields, width), F32), [SM, VM], name="pick"
    )(table, returned)
    parts = lax.all_to_all(terms, "member", 0, 0, tiled=True)
    return call(
        final_kernel, (sds(state.shape, F32), sds(state.shape, F32)), [SM] + [VM] * 8, (ANY, ANY),
        scratch=[pltpu.VMEM(state.shape, F32), pltpu.VMEM(state.shape, F32), pltpu.SemaphoreType.DMA((2, 3))],
        name="final",
    )(diffusivity, cells, parts, base, velocity, *halos)


def solution(mesh):
    team, member = mesh.devices.shape
    own_mesh = Mesh(mesh.devices.reshape(team // 2, 2, member), ("z", "core", "member"))
    line = ("z", "core")
    tile = P(None, line, "member")
    weight = P(line, "member", None, None)
    return jax.shard_map(
        shards,
        mesh=own_mesh,
        in_specs=(tile, tile, tile, P(), P((*line, "member"), None), P(), weight, weight, weight, weight),
        out_specs=(tile, tile),
        check_vma=False,
    )
```

```python
import jax
import jax.numpy as jnp
from jax import lax
from jax.experimental import pallas as pl
from jax.experimental.pallas import tpu as pltpu
from jax.sharding import Mesh, PartitionSpec as P


BF = jnp.bfloat16
F32 = jnp.float32
I32 = jnp.int32
TIME_STEP = 0.25
VM = pl.BlockSpec(memory_space=pltpu.VMEM)
SM = pl.BlockSpec(memory_space=pltpu.SMEM)

ANY = pl.BlockSpec(memory_space=pl.ANY)

SRC, POS, OWN, SIB, N_OWN, N_SIB = 0, 32, 48, 64, 80, 81


def dot(a, b, dims=((1,), (0,))):
    return lax.dot_general(a, b, (dims, ((), ())), preferred_element_type=F32)


def silu(x):
    return (x * lax.logistic(x)).astype(BF)


def in_hbm(array):
    return pltpu.with_memory_space_constraint(array, pltpu.HBM)


def iota(shape, dim):
    return lax.broadcasted_iota(I32, shape, dim)


def make_table(team_ref):
    z, c = lax.axis_index("z"), lax.axis_index("core")
    n = team_ref.shape[1]
    across = jnp.broadcast_to(team_ref[...].astype(F32), (n, n))
    down = across.T
    row, lane = iota((n, n), 0), iota((n, n), 1)
    before = (across == down) & (lane < row)
    rank = jnp.sum(jnp.where(before, 1.0, 0.0), axis=1, keepdims=True).astype(I32)
    shape = (n, 128)
    g = down[:, :128].astype(I32)
    rank = jnp.broadcast_to(rank, shape)
    b, s = iota(shape, 0), iota(shape, 1)
    core = (rank + g) & 1
    place = ((g >> 1) * 2 + core) * 2 + (g & 1)
    arrives = (b >> 4) * 2 + (g & 1)
    here = (b >> 4) == 2 * z + c
    own = (core == c) & (g == 2 * z + c)
    sib = (core == c) & (g == 2 * z + 1 - c)
    value = jnp.where((s < POS) & here & (place == s), b & 15, jnp.zeros(shape, I32))
    value = jnp.where((s >= POS) & (s < OWN) & here & ((b & 15) == s - POS), place, value)
    value = jnp.where((s >= OWN) & (s < SIB) & own & ((rank >> 1) == s - OWN), arrives, value)
    value = jnp.where((s >= SIB) & (s < N_OWN) & sib & ((rank >> 1) == s - SIB), arrives, value)
    value = jnp.where((s == N_OWN) & own, 1, value)
    value = jnp.where((s == N_SIB) & sib, 1, value)
    return jnp.sum(value.astype(F32), axis=0, keepdims=True).astype(I32)


def front_kernel(team_hbm, cells_hbm, state_hbm, *refs):
    table, blocks, x_low, x_high, y_low, y_high, team, cells, state, own, sems, out_sems = refs
    fields, rows, cols = state.shape
    width = cells.shape[1]
    parts = sems.shape[0] - 2
    some = fields // parts
    load_team = pltpu.make_async_copy(team_hbm, team, sems.at[parts + 1])
    load_team.start()
    loads = [pltpu.make_async_copy(cells_hbm, cells, sems.at[parts])]
    for k in range(parts):
        at = pl.ds(k * some, some)
        loads.append(pltpu.make_async_copy(state_hbm.at[at], state.at[at], sems.at[k]))
    for load in loads:
        load.start()
    loads[0].wait()
    column = cells[...] & (cols - 1)
    line = cells[...] >> (cols.bit_length() - 1)
    picks = jnp.where(iota((cols, width), 0) == column, 1.0, 0.0).astype(BF)
    at_row = (iota((rows, width), 0) == line)[None]
    e, j = iota((16, cols), 0), iota((16, cols), 1)
    ends = jnp.where(((e == 0) & (j == 0)) | ((e == 1) & (j == cols - 1)), 1.0, 0.0).astype(BF)
    load_team.wait()
    table[...] = make_table(team)
    found_in = []
    for k in range(parts):
        loads[k + 1].wait()
        values = state[k * some : (k + 1) * some].astype(BF)
        flat = values.reshape(some * rows, cols)
        found = dot(flat, picks).reshape(some, rows, width)
        found_in.append(jnp.sum(jnp.where(at_row, found, 0.0), axis=1))
    own[...] = jnp.concatenate(found_in, axis=0).astype(BF)
    sends = [pltpu.make_async_copy(own, blocks.at[k], out_sems.at[k]) for k in range(blocks.shape[0])]
    for send in sends:
        send.start()
    x_low[...] = state[:, 0, :].astype(BF)
    x_high[...] = state[:, rows - 1, :].astype(BF)
    sides = dot(ends, state[...].astype(BF).reshape(fields * rows, cols), ((1,), (1,))).astype(BF)
    y_low[...], y_high[...] = sides[0:1], sides[1:2]
    for send in sends:
        send.wait()


def select_kernel(base, table, rows, out):
    for k in range(out.shape[0]):
        out[k] = rows[table[0, base + k]]


def network_kernel(table, x, *refs):
    out, rates, sems, load_sems = refs[8], refs[9], refs[10], refs[11]
    partner, own = [refs[4], refs[5], refs[16], refs[7]], refs[12:16]
    first_load = pltpu.make_async_copy(refs[6], refs[16], load_sems.at[4])
    loads = [pltpu.make_async_copy(refs[k], own[k], load_sems.at[k]) for k in range(4)]
    for load in (first_load, *loads):
        load.start()

    def copy_of(w, p, a):
        return pltpu.make_async_copy(rates.at[w, p], out.at[a], sems.at[w, p])

    def group(weights, w, first, n, start, size, before_low=None):
        w_in, w_mid, w_low, w_out = weights
        at = [table[0, first + jnp.minimum(start + i, n - 1)] for i in range(size)]
        states = jnp.concatenate([x[i] for i in at], axis=1)
        one = silu(dot(w_in[...], states, ((0,), (0,))))
        two = silu(dot(w_mid[...], one))
        if before_low is not None:
            before_low()
        three = silu(dot(w_low[...], two))
        found = dot(w_out[...], three)
        for i, a in enumerate(at):
            rates[w, start + i] = found[:, i * 128 : (i + 1) * 128]

            @pl.when(start + i < n)
            def _(i=i, a=a):
                copy_of(w, start + i, a).start()

    counts = table[0, N_SIB], table[0, N_OWN]
    for w, (weights, first) in enumerate(((partner, SIB), (own, OWN))):
        n = counts[w]
        full = (n + 3) // 8
        if w == 0:

            @pl.when(full > 0)
            def _(n=n):
                group(partner, 0, SIB, n, 0, 8, first_load.wait)

            @pl.when(full == 0)
            def _():
                first_load.wait()

        else:
            for load in loads:
                load.wait()

        def step(k, _, weights=weights, w=w, first=first, n=n):
            group(weights, w, first, n, 8 * k, 8)
            return 0

        lax.fori_loop(1 - w, full, step, 0)

        @pl.when(n > 8 * full)
        def _(weights=weights, w=w, first=first, n=n, full=full):
            group(weights, w, first, n, 8 * full, 4)

    for w in range(2):
        for p in range(16):

            @pl.when(p < counts[w])
            def _(w=w, p=p):
                copy_of(w, p, 0).wait()


def base_kernel(diff, start, state, velocity, out):
    fields, rows, cols = state.shape
    row, lane = iota((rows, cols), 0), iota((rows, cols), 1)
    half_x, half_y = 0.5 * velocity[0], 0.5 * velocity[1]
    for f in range(fields):
        u = state[f]
        plus_x = jnp.where(row == rows - 1, 0.0, pltpu.roll(u, rows - 1, 0))
        minus_x = jnp.where(row == 0, 0.0, pltpu.roll(u, 1, 0))
        plus_y = jnp.where(lane == cols - 1, 0.0, pltpu.roll(u, cols - 1, 1))
        minus_y = jnp.where(lane == 0, 0.0, pltpu.roll(u, 1, 1))
        flow = diff[f] * (plus_x + minus_x + plus_y + minus_y - 4.0 * u)
        flow = flow - half_x * (plus_x - minus_x) - half_y * (plus_y - minus_y)
        out[f] = 0.75 * start[f] + 0.25 * (u + TIME_STEP * flow)


def final_kernel(diff, cells, parts, base, velocity, up, down, left, right, source, new, source_tile, new_tile, sems):
    fields, rows, cols = base.shape
    width = cells.shape[1]
    rates = parts[0]
    for n in range(1, parts.shape[0]):
        rates = rates + parts[n]
    high = rates.astype(BF).astype(F32)
    low = rates - high
    column = cells[...] & (cols - 1)
    line = cells[...] >> (cols.bit_length() - 1)
    at_row = iota((rows, width), 0) == line
    at_col = jnp.where(iota((cols, width), 0) == column, 1.0, 0.0).astype(BF)
    at_col = jnp.concatenate([at_col, at_col], axis=1)
    some = fields // sems.shape[1]
    copies = []
    scale = 0.25 * TIME_STEP
    e, j = iota((2, cols), 0), iota((2, cols), 1)
    ends = jnp.where(((e == 0) & (j == 0)) | ((e == 1) & (j == cols - 1)), 1.0, 0.0).astype(BF)
    edges = jnp.concatenate([left[...], right[...]], axis=0)
    sides = dot(edges, ends, ((0,), (0,))).reshape(fields, rows, cols)
    lane = iota((rows, cols), 1)
    along = jnp.where(lane == 0, 0.5, -0.5) * velocity[1]
    low_x, high_x = 0.5 * velocity[0, 0:1, :], -0.5 * velocity[0, rows - 1 : rows, :]
    for k in range(sems.shape[1]):
        spread = []
        for f in range(k * some, (k + 1) * some):
            left = jnp.where(at_row, high[f : f + 1], 0.0)
            right = jnp.where(at_row, low[f : f + 1], 0.0)
            spread.append(jnp.concatenate([left, right], axis=1).astype(BF))
        placed = dot(jnp.concatenate(spread, axis=0), at_col, ((1,), (1,)))
        placed = placed.reshape(some, rows, cols)
        part = pl.ds(k * some, some)
        source_tile[part] = placed
        for f in range(some):
            g = k * some + f
            new_tile[g] = base[g] + scale * (placed[f] + (diff[g] + along) * sides[g])
            above, below = up[g : g + 1].astype(F32), down[g : g + 1].astype(F32)
            new_tile[g, 0:1] = new_tile[g, 0:1] + scale * (diff[g] + low_x) * above
            new_tile[g, rows - 1 : rows] = new_tile[g, rows - 1 : rows] + scale * (diff[g] + high_x) * below
        for i, (tile, out) in enumerate(((source_tile, source), (new_tile, new))):
            copies.append(pltpu.make_async_copy(tile.at[part], out.at[part], sems.at[i, k]))
            copies[-1].start()
    for copy in copies:
        copy.wait()


def call(body, out_shape, in_specs, out_specs=None, scratch=(), mib=8):
    if out_specs is None:
        out_specs = jax.tree.map(lambda _: VM, out_shape)
    return pl.pallas_call(
        body, out_shape=out_shape, in_specs=in_specs, out_specs=out_specs,
        scratch_shapes=scratch, compiler_params=pltpu.CompilerParams(vmem_limit_bytes=mib * 2**20),
    )


def shards(start, state, velocity, diffusivity, cells, block_team, w_in, w_mid, w_low, w_out):
    fields, rows, cols = state.shape
    width = cells.shape[1]
    sds = jax.ShapeDtypeStruct
    members = lax.axis_size("member")
    teams = lax.axis_size("z") * lax.axis_size("core")
    up = [(i, (i + 1) % 16) for i in range(16)]
    back = [(b, a) for a, b in up]
    swap = [(0, 1), (1, 0)]
    line = ("z", "core")

    weights = [w_in[0, 0].T, w_mid[0, 0], w_low[0, 0], w_out[0, 0]]
    edge = sds((1, fields * rows), BF)
    team = block_team.T
    table, blocks, x_low, x_high, y_low, y_high = call(
        front_kernel,
        (sds((1, 128), I32), sds((members, fields, width), BF), sds((fields, cols), BF), sds((fields, cols), BF), edge, edge),
        [ANY] * 3, (VM, ANY, VM, VM, VM, VM),
        scratch=[pltpu.VMEM(team.shape, I32), pltpu.VMEM(cells.shape, I32), pltpu.VMEM(state.shape, F32), pltpu.VMEM((fields, width), BF),
                 pltpu.SemaphoreType.DMA((5,)), pltpu.SemaphoreType.DMA((members,))],
    )(in_hbm(team), in_hbm(cells), in_hbm(state))
    blocks, *sent = lax.optimization_barrier((blocks, *weights))
    gathered = lax.all_to_all(blocks, "member", 0, 0, tiled=True)
    partner = [lax.ppermute(sent[k], "core", swap) for k in (0, 3)]
    partner[1:1] = [lax.ppermute(sent[k], "core", swap) for k in (1, 2)]
    gathered, partner[0], partner[3] = lax.optimization_barrier((gathered, partner[0], partner[3]))
    outgoing = call(lambda *r: select_kernel(SRC, *r), sds((2 * teams, fields, width), BF), [SM, VM])(table, gathered)
    incoming = lax.all_to_all(outgoing, line, 0, 0, tiled=True)

    produced = call(
        network_kernel, sds((2 * teams, fields, width), F32), [SM, VM] + [ANY] * 4 + [VM, VM, ANY, VM], ANY,
        scratch=[pltpu.VMEM((2, 16, fields, width), F32), pltpu.SemaphoreType.DMA((2, 16)), pltpu.SemaphoreType.DMA((5,))]
        + [pltpu.VMEM(w.shape, BF) for w in (*weights, weights[2])],
        mib=32,
    )(table, incoming, *[in_hbm(w) for w in weights], partner[0], partner[1], in_hbm(partner[2]), partner[3])
    produced, x_low, x_high, y_low, y_high = lax.optimization_barrier((produced, x_low, x_high, y_low, y_high))
    returned = lax.all_to_all(produced, line, 0, 0, tiled=True)
    halos = (
        lax.ppermute(x_high, line, up),
        lax.ppermute(x_low, line, back),
        lax.ppermute(y_high, "member", up),
        lax.ppermute(y_low, "member", back),
    )
    base = call(base_kernel, sds(state.shape, F32), [SM] + [VM] * 3)(
        diffusivity, in_hbm(start), in_hbm(state), in_hbm(velocity)
    )
    returned, base, *halos = lax.optimization_barrier((returned, base, *halos))
    terms = call(lambda *r: select_kernel(POS, *r), sds((members, fields, width), F32), [SM, VM])(table, returned)
    parts = lax.all_to_all(terms, "member", 0, 0, tiled=True)
    return call(
        final_kernel, (sds(state.shape, F32), sds(state.shape, F32)), [SM] + [VM] * 8, (ANY, ANY),
        scratch=[pltpu.VMEM(state.shape, F32), pltpu.VMEM(state.shape, F32), pltpu.SemaphoreType.DMA((2, 3))],
    )(diffusivity, cells, parts, base, velocity, *halos)


def solution(mesh):
    team, member = mesh.devices.shape
    own_mesh = Mesh(mesh.devices.reshape(team // 2, 2, member), ("z", "core", "member"))
    line = ("z", "core")
    tile = P(None, line, "member")
    weight = P(line, "member", None, None)
    return jax.shard_map(
        shards,
        mesh=own_mesh,
        in_specs=(tile, tile, tile, P(), P((*line, "member"), None), P(), weight, weight, weight, weight),
        out_specs=(tile, tile),
        check_vma=False,
    )
```

```python
import jax
import jax.numpy as jnp
from jax import lax
from jax.experimental import pallas as pl
from jax.experimental.pallas import tpu as pltpu
from jax.sharding import Mesh, PartitionSpec as P


BF = jnp.bfloat16
F32 = jnp.float32
I32 = jnp.int32
TIME_STEP = 0.25
VM = pl.BlockSpec(memory_space=pltpu.VMEM)
SM = pl.BlockSpec(memory_space=pltpu.SMEM)

ANY = pl.BlockSpec(memory_space=pl.ANY)

SRC, POS, OWN, SIB, N_OWN, N_SIB = 0, 32, 48, 64, 80, 81


def dot(a, b, dims=((1,), (0,))):
    return lax.dot_general(a, b, (dims, ((), ())), preferred_element_type=F32)


def silu(x):
    return (x * lax.logistic(x)).astype(BF)


def in_hbm(array):
    return pltpu.with_memory_space_constraint(array, pltpu.HBM)


def iota(shape, dim):
    return lax.broadcasted_iota(I32, shape, dim)


def make_table(team_ref):
    z, c = lax.axis_index("z"), lax.axis_index("core")
    n = team_ref.shape[1]
    across = jnp.broadcast_to(team_ref[...].astype(F32), (n, n))
    down = across.T
    row, lane = iota((n, n), 0), iota((n, n), 1)
    before = (across == down) & (lane < row)
    rank = jnp.sum(jnp.where(before, 1.0, 0.0), axis=1, keepdims=True).astype(I32)
    shape = (n, 128)
    g = down[:, :128].astype(I32)
    rank = jnp.broadcast_to(rank, shape)
    b, s = iota(shape, 0), iota(shape, 1)
    core = (rank + g) & 1
    place = ((g >> 1) * 2 + core) * 2 + (g & 1)
    arrives = (b >> 4) * 2 + (g & 1)
    here = (b >> 4) == 2 * z + c
    own = (core == c) & (g == 2 * z + c)
    sib = (core == c) & (g == 2 * z + 1 - c)
    value = jnp.where((s < POS) & here & (place == s), b & 15, jnp.zeros(shape, I32))
    value = jnp.where((s >= POS) & (s < OWN) & here & ((b & 15) == s - POS), place, value)
    value = jnp.where((s >= OWN) & (s < SIB) & own & ((rank >> 1) == s - OWN), arrives, value)
    value = jnp.where((s >= SIB) & (s < N_OWN) & sib & ((rank >> 1) == s - SIB), arrives, value)
    value = jnp.where((s == N_OWN) & own, 1, value)
    value = jnp.where((s == N_SIB) & sib, 1, value)
    return jnp.sum(value.astype(F32), axis=0, keepdims=True).astype(I32)


def front_kernel(team_hbm, cells_hbm, state_hbm, *refs):
    table, blocks, x_low, x_high, y_low, y_high, team, cells, state, own, sems, out_sems = refs
    fields, rows, cols = state.shape
    width = cells.shape[1]
    parts = sems.shape[0] - 2
    some = fields // parts
    load_team = pltpu.make_async_copy(team_hbm, team, sems.at[parts + 1])
    load_team.start()
    loads = [pltpu.make_async_copy(cells_hbm, cells, sems.at[parts])]
    for k in range(parts):
        at = pl.ds(k * some, some)
        loads.append(pltpu.make_async_copy(state_hbm.at[at], state.at[at], sems.at[k]))
    for load in loads:
        load.start()
    loads[0].wait()
    column = cells[...] & (cols - 1)
    line = cells[...] >> (cols.bit_length() - 1)
    picks = jnp.where(iota((cols, width), 0) == column, 1.0, 0.0).astype(BF)
    at_row = (iota((rows, width), 0) == line)[None]
    e, j = iota((16, cols), 0), iota((16, cols), 1)
    ends = jnp.where(((e == 0) & (j == 0)) | ((e == 1) & (j == cols - 1)), 1.0, 0.0).astype(BF)
    load_team.wait()
    table[...] = make_table(team)
    found_in = []
    for k in range(parts):
        loads[k + 1].wait()
        values = state[k * some : (k + 1) * some].astype(BF)
        flat = values.reshape(some * rows, cols)
        found = dot(flat, picks).reshape(some, rows, width)
        found_in.append(jnp.sum(jnp.where(at_row, found, 0.0), axis=1))
    own[...] = jnp.concatenate(found_in, axis=0).astype(BF)
    sends = [pltpu.make_async_copy(own, blocks.at[k], out_sems.at[k]) for k in range(blocks.shape[0])]
    for send in sends:
        send.start()
    x_low[...] = state[:, 0, :].astype(BF)
    x_high[...] = state[:, rows - 1, :].astype(BF)
    sides = dot(ends, state[...].astype(BF).reshape(fields * rows, cols), ((1,), (1,))).astype(BF)
    y_low[...], y_high[...] = sides[0:1], sides[1:2]
    for send in sends:
        send.wait()


def select_kernel(base, table, rows, out):
    for k in range(out.shape[0]):
        out[k] = rows[table[0, base + k]]


def network_kernel(table, x, *refs):
    out, rates, sems, load_sems = refs[8], refs[9], refs[10], refs[11]
    partner, own = [refs[4], refs[5], refs[16], refs[7]], refs[12:16]
    first_load = pltpu.make_async_copy(refs[6], refs[16], load_sems.at[4])
    loads = [pltpu.make_async_copy(refs[k], own[k], load_sems.at[k]) for k in range(4)]
    for load in (first_load, *loads):
        load.start()

    def copy_of(w, p, a):
        return pltpu.make_async_copy(rates.at[w, p], out.at[a], sems.at[w, p])

    def group(weights, w, first, n, start, size, before_low=None):
        w_in, w_mid, w_low, w_out = weights
        at = [table[0, first + jnp.minimum(start + i, n - 1)] for i in range(size)]
        states = jnp.concatenate([x[i] for i in at], axis=1)
        one = silu(dot(w_in[...], states, ((0,), (0,))))
        half = w_mid.shape[0] // 2
        two = jnp.concatenate([silu(dot(w_mid[:half], one)), silu(dot(w_mid[half:], one))], axis=0)
        if before_low is not None:
            before_low()
        three = silu(dot(w_low[...], two))
        found = dot(w_out[...], three)
        for i, a in enumerate(at):
            rates[w, start + i] = found[:, i * 128 : (i + 1) * 128]

            @pl.when(start + i < n)
            def _(i=i, a=a):
                copy_of(w, start + i, a).start()

    counts = table[0, N_SIB], table[0, N_OWN]
    for w, (weights, first) in enumerate(((partner, SIB), (own, OWN))):
        n = counts[w]
        full = (n + 3) // 8
        if w == 0:

            @pl.when(full > 0)
            def _(n=n):
                group(partner, 0, SIB, n, 0, 8, first_load.wait)

            @pl.when(full == 0)
            def _():
                first_load.wait()

        else:
            for load in loads:
                load.wait()

        def step(k, _, weights=weights, w=w, first=first, n=n):
            group(weights, w, first, n, 8 * k, 8)
            return 0

        lax.fori_loop(1 - w, full, step, 0)

        @pl.when(n > 8 * full)
        def _(weights=weights, w=w, first=first, n=n, full=full):
            group(weights, w, first, n, 8 * full, 4)

    for w in range(2):
        for p in range(16):

            @pl.when(p < counts[w])
            def _(w=w, p=p):
                copy_of(w, p, 0).wait()


def base_kernel(diff, start, state, velocity, out, spread):
    fields, rows, cols = state.shape
    row, lane = iota((rows, cols), 0), iota((rows, cols), 1)
    half_x, half_y = 0.5 * velocity[0], 0.5 * velocity[1]
    for f in range(fields):
        u = state[f]
        plus_x = jnp.where(row == rows - 1, 0.0, pltpu.roll(u, rows - 1, 0))
        minus_x = jnp.where(row == 0, 0.0, pltpu.roll(u, 1, 0))
        plus_y = jnp.where(lane == cols - 1, 0.0, pltpu.roll(u, cols - 1, 1))
        minus_y = jnp.where(lane == 0, 0.0, pltpu.roll(u, 1, 1))
        flow = diff[f] * (plus_x + minus_x + plus_y + minus_y - 4.0 * u)
        flow = flow - half_x * (plus_x - minus_x) - half_y * (plus_y - minus_y)
        out[f] = 0.75 * start[f] + 0.25 * (u + TIME_STEP * flow)
        spread[f : f + 1] = jnp.full((1, cols), diff[f], F32)


def final_kernel(diff, cells, parts, base, velocity, up, down, left, right, source, new, source_tile, new_tile, sems):
    fields, rows, cols = base.shape
    width = cells.shape[1]
    rates = parts[0]
    for n in range(1, parts.shape[0]):
        rates = rates + parts[n]
    high = rates.astype(BF).astype(F32)
    low = rates - high
    column = cells[...] & (cols - 1)
    line = cells[...] >> (cols.bit_length() - 1)
    at_row = iota((rows, width), 0) == line
    at_col = jnp.where(iota((cols, width), 0) == column, 1.0, 0.0).astype(BF)
    at_col = jnp.concatenate([at_col, at_col], axis=1)
    some = fields // sems.shape[1]
    copies = []
    scale = 0.25 * TIME_STEP
    e, j = iota((2, cols), 0), iota((2, cols), 1)
    ends = jnp.where(((e == 0) & (j == 0)) | ((e == 1) & (j == cols - 1)), 1.0, 0.0).astype(BF)
    edges = jnp.concatenate([left[...], right[...]], axis=0)
    sides = dot(edges, ends, ((0,), (0,))).reshape(fields, rows, cols)
    lane = iota((rows, cols), 1)
    along = jnp.where(lane == 0, 0.5, -0.5) * velocity[1]
    low_x, high_x = 0.5 * velocity[0, 0:1, :], -0.5 * velocity[0, rows - 1 : rows, :]
    for k in range(sems.shape[1]):
        spread = []
        for f in range(k * some, (k + 1) * some):
            left = jnp.where(at_row, high[f : f + 1], 0.0)
            right = jnp.where(at_row, low[f : f + 1], 0.0)
            spread.append(jnp.concatenate([left, right], axis=1).astype(BF))
        placed = dot(jnp.concatenate(spread, axis=0), at_col, ((1,), (1,)))
        placed = placed.reshape(some, rows, cols)
        part = pl.ds(k * some, some)
        source_tile[part] = placed
        for f in range(some):
            g = k * some + f
            new_tile[g] = base[g] + scale * (placed[f] + (diff[g : g + 1] + along) * sides[g])
            above, below = up[g : g + 1].astype(F32), down[g : g + 1].astype(F32)
            new_tile[g, 0:1] = new_tile[g, 0:1] + scale * (diff[g : g + 1] + low_x) * above
            new_tile[g, rows - 1 : rows] = new_tile[g, rows - 1 : rows] + scale * (diff[g : g + 1] + high_x) * below
        for i, (tile, out) in enumerate(((source_tile, source), (new_tile, new))):
            copies.append(pltpu.make_async_copy(tile.at[part], out.at[part], sems.at[i, k]))
            copies[-1].start()
    for copy in copies:
        copy.wait()


def call(body, out_shape, in_specs, out_specs=None, scratch=(), mib=8):
    if out_specs is None:
        out_specs = jax.tree.map(lambda _: VM, out_shape)
    return pl.pallas_call(
        body, out_shape=out_shape, in_specs=in_specs, out_specs=out_specs,
        scratch_shapes=scratch, compiler_params=pltpu.CompilerParams(vmem_limit_bytes=mib * 2**20),
    )


def shards(start, state, velocity, diffusivity, cells, block_team, w_in, w_mid, w_low, w_out):
    fields, rows, cols = state.shape
    width = cells.shape[1]
    sds = jax.ShapeDtypeStruct
    members = lax.axis_size("member")
    teams = lax.axis_size("z") * lax.axis_size("core")
    up = [(i, (i + 1) % 16) for i in range(16)]
    back = [(b, a) for a, b in up]
    swap = [(0, 1), (1, 0)]
    line = ("z", "core")

    weights = [w_in[0, 0].T, w_mid[0, 0], w_low[0, 0], w_out[0, 0]]
    edge = sds((1, fields * rows), BF)
    team = block_team.T
    table, blocks, x_low, x_high, y_low, y_high = call(
        front_kernel,
        (sds((1, 128), I32), sds((members, fields, width), BF), sds((fields, cols), BF), sds((fields, cols), BF), edge, edge),
        [ANY] * 3, (VM, ANY, VM, VM, VM, VM),
        scratch=[pltpu.VMEM(team.shape, I32), pltpu.VMEM(cells.shape, I32), pltpu.VMEM(state.shape, F32), pltpu.VMEM((fields, width), BF),
                 pltpu.SemaphoreType.DMA((5,)), pltpu.SemaphoreType.DMA((members,))],
    )(in_hbm(team), in_hbm(cells), in_hbm(state))
    blocks, *sent = lax.optimization_barrier((blocks, *weights))
    gathered = lax.all_to_all(blocks, "member", 0, 0, tiled=True)
    partner = [lax.ppermute(sent[k], "core", swap) for k in (0, 3)]
    partner[1:1] = [lax.ppermute(sent[k], "core", swap) for k in (1, 2)]
    gathered, partner[0], partner[3] = lax.optimization_barrier((gathered, partner[0], partner[3]))
    outgoing = call(lambda *r: select_kernel(SRC, *r), sds((2 * teams, fields, width), BF), [SM, VM])(table, gathered)
    incoming = lax.all_to_all(outgoing, line, 0, 0, tiled=True)

    produced = call(
        network_kernel, sds((2 * teams, fields, width), F32), [SM, VM] + [ANY] * 4 + [VM, VM, ANY, VM], ANY,
        scratch=[pltpu.VMEM((2, 16, fields, width), F32), pltpu.SemaphoreType.DMA((2, 16)), pltpu.SemaphoreType.DMA((5,))]
        + [pltpu.VMEM(w.shape, BF) for w in (*weights, weights[2])],
        mib=32,
    )(table, incoming, *[in_hbm(w) for w in weights], partner[0], partner[1], in_hbm(partner[2]), partner[3])
    produced, x_low, x_high, y_low, y_high = lax.optimization_barrier((produced, x_low, x_high, y_low, y_high))
    returned = lax.all_to_all(produced, line, 0, 0, tiled=True)
    halos = (
        lax.ppermute(x_high, line, up),
        lax.ppermute(x_low, line, back),
        lax.ppermute(y_high, "member", up),
        lax.ppermute(y_low, "member", back),
    )
    base, spread = call(base_kernel, (sds(state.shape, F32), sds((fields, cols), F32)), [SM] + [VM] * 3)(
        diffusivity, in_hbm(start), in_hbm(state), in_hbm(velocity)
    )
    returned, base, *halos = lax.optimization_barrier((returned, base, *halos))
    terms = call(lambda *r: select_kernel(POS, *r), sds((members, fields, width), F32), [SM, VM])(table, returned)
    parts = lax.all_to_all(terms, "member", 0, 0, tiled=True)
    return call(
        final_kernel, (sds(state.shape, F32), sds(state.shape, F32)), [VM] * 9, (ANY, ANY),
        scratch=[pltpu.VMEM(state.shape, F32), pltpu.VMEM(state.shape, F32), pltpu.SemaphoreType.DMA((2, 4))],
    )(spread, cells, parts, base, velocity, *halos)


def solution(mesh):
    team, member = mesh.devices.shape
    own_mesh = Mesh(mesh.devices.reshape(team // 2, 2, member), ("z", "core", "member"))
    line = ("z", "core")
    tile = P(None, line, "member")
    weight = P(line, "member", None, None)
    return jax.shard_map(
        shards,
        mesh=own_mesh,
        in_specs=(tile, tile, tile, P(), P((*line, "member"), None), P(), weight, weight, weight, weight),
        out_specs=(tile, tile),
        check_vma=False,
    )
```
